256 devices in a mesh: rows: 256 (over y, x, z, core).
Axes of the slice: x: 4, y: 4, z: 8, core: 2. Of those that a mesh axis runs over, the one named last changes fastest.
Arguments:
- source: float32 [64, 1048576], P(None, 'rows'), may hold values from -6 to 6
- band_values: float32 [128, 1048576], P(None, 'rows'), may hold values from -0.625 to 0.625
- offsets: int32 [128], replicated, may hold values from -128 to 128, as said below
Outputs:
- compressed: float32 [128, 1048576], P(None, 'rows')
The draws below stay inside these ranges and needn't reach their ends.
Inputs may be any that keep to these rules, and one draw needn't show every extreme that they name: The 128 offsets are distinct and include both -128 and 128.
All inputs are finite; a program needn't handle non-finite values.
Results may differ from the reference program's by a relative error of at most 0.0003.
Values sent between devices are 32-bit elements; how exact they have to be, the bound alone decides.
No kernel may reach another device: no remote copies, remote signals or barrier semaphores. Data moves between devices by JAX's collectives and lax.ppermute only.
A program may use at most 192 MiB of HBM per device.

```python
import jax
import jax.numpy as jnp
from jax import lax

ROWS_DEV = 4096
HB = 128
NB = 128
RB = 64
K1 = 128
K2 = 128
N = 1048576
N_ROWS = 256


def draw_offsets(key, part):
    inner = jax.random.permutation(jax.random.fold_in(key, 11), 2 * HB - 1)[:NB - 2] - (HB - 1)
    ends = jnp.array([-HB, HB], jnp.int32)
    return jnp.concatenate([ends, inner.astype(jnp.int32)])


def steps_of(rng, dims, split, smallest, largest):
    gain, own = 1.0, jax.random.fold_in(rng, 6)
    for axis_at, parts in split:
        steps = jnp.exp(jax.random.uniform(jax.random.fold_in(own, axis_at), (parts,), jnp.float32, smallest / len(split), largest / len(split)))
        gain = gain * jnp.repeat(steps, dims[axis_at] // parts).reshape([-1 if axis == axis_at else 1 for axis in range(len(dims))])
    return gain


def bell_draw(own_key, dims, deviation, reach, split=(), kind=jnp.bfloat16):
    values = deviation * jax.random.normal(own_key, dims, jnp.float32)
    if split:
        values = values * steps_of(own_key, dims, split, -0.22, 0.18)
    return jnp.clip(values, -reach, reach).astype(kind)


def setup_inputs(seed: int = 0) -> dict:
    keys = jax.random.split(jax.random.key(seed), 4)
    source = bell_draw(keys[0], (RB, N), 1.0, 6.0, ((1, 256),), jnp.float32)
    band_values = bell_draw(keys[1], (NB, N), (0.5 / NB ** 0.5), 0.625, ((1, 256),), jnp.float32)
    offsets = draw_offsets(jax.random.fold_in(keys[3], 71), 0)
    return dict(source=source, band_values=band_values, offsets=offsets)


def band_blocks(band_values, offsets):
    diagonals = band_values.shape[0]
    blocks = band_values.shape[1] // HB
    values = band_values.reshape(diagonals, blocks, HB).transpose(1, 0, 2)
    within = jnp.arange(HB, dtype=jnp.int32)
    columns = within[None, :] + offsets[:, None].astype(jnp.int32) + HB
    row_index = jnp.broadcast_to(within[None, :], columns.shape)
    blocked = jnp.zeros((blocks, HB, 3 * HB), values.dtype)
    return blocked.at[:, row_index, columns].set(values)

def apply_band(extended, blocked):
    width = extended.shape[0]
    blocks = blocked.shape[0]
    pieces = extended.reshape(width, blocks + 2, HB)
    windows = jnp.concatenate([pieces[:, :-2], pieces[:, 1:-1], pieces[:, 2:]], axis=2)
    result = jnp.einsum('cbj,brj->cbr', windows, blocked, precision=lax.Precision.HIGHEST)
    return result.reshape(width, blocks * HB)

def apply_all(factor, band_values, offsets):
    width = factor.shape[0]
    padded = jnp.pad(factor, ((0, 0), (HB, HB)))

    def slab(index):
        start = (index * ROWS_DEV).astype(jnp.int32)
        anchor = jnp.zeros((), jnp.int32)
        piece = lax.dynamic_slice(padded, (anchor, start), (width, ROWS_DEV + 2 * HB))
        values = lax.dynamic_slice(band_values, (anchor, start), (band_values.shape[0], ROWS_DEV))
        return apply_band(piece, band_blocks(values, offsets))
    stacked = lax.map(slab, jnp.arange(N_ROWS, dtype=jnp.int32))
    return stacked.transpose(1, 0, 2).reshape(width, N_ROWS * ROWS_DEV)

def compress(grammian, retain):
    spanning = grammian[:, :retain]
    coeffs = None
    for repeat in range(2):
        if repeat > 0:
            spanning = jnp.dot(grammian, coeffs.T, precision=lax.Precision.HIGHEST)
        mapped = jnp.dot(grammian, spanning, precision=lax.Precision.HIGHEST)
        metric = jnp.dot(spanning.T, mapped, precision=lax.Precision.HIGHEST)
        metric = 0.5 * (metric + metric.T)
        factor = jnp.linalg.cholesky(metric)
        coeffs = jax.scipy.linalg.solve_triangular(factor, spanning.T, lower=True)
    return coeffs

def reference(source, band_values, offsets):
    total = source.shape[1]
    first = jnp.concatenate([source, apply_all(source, band_values, offsets)], axis=0)
    gram_one = jnp.dot(first, first.T, precision=lax.Precision.HIGHEST) / total
    coeffs_one = compress(gram_one, K1)
    factor = jnp.dot(coeffs_one, first, precision=lax.Precision.HIGHEST)
    once_more = apply_all(factor, band_values, offsets)
    squared = apply_all(once_more, band_values, offsets)
    second = jnp.concatenate([factor, squared], axis=0)
    gram_two = jnp.dot(second, second.T, precision=lax.Precision.HIGHEST) / total
    coeffs_two = compress(gram_two, K2)
    return jnp.dot(coeffs_two, second, precision=lax.Precision.HIGHEST)
```

```python
import functools

import jax
import jax.numpy as jnp
from jax import lax
from jax.experimental import pallas as pl
from jax.experimental.pallas import tpu as pltpu
from jax.sharding import PartitionSpec as P

HB = 128
WB = 256
NT = (((1,), (1,)), ((), ()))
TN = (((0,), (0,)), ((), ()))


def split(x):
    high = x.astype(jnp.bfloat16)
    return high, (x - high.astype(jnp.float32)).astype(jnp.bfloat16)


def mm(a, b, dims=(((1,), (0,)), ((), ()))):
    return lax.dot_general(a, b, dims, preferred_element_type=jnp.float32)


def exact(a, b, dims=(((1,), (0,)), ((), ()))):
    return lax.dot_general(
        a, b, dims, precision=lax.Precision.HIGHEST, preferred_element_type=jnp.float32
    )


def powers_kernel(total, src_ref, band_ref, off_ref, high_ref, low_ref, gram_ref, xh, xl, wh, wl):
    rows = src_ref.shape[0]
    width = high_ref.shape[1]
    blocks = width // WB + 2
    diagonals = off_ref.shape[0]
    span = 2 * WB
    lanes = lax.broadcasted_iota(jnp.int32, (diagonals, span), 1)
    pick = jnp.where(lanes == off_ref[...] + HB, 1.0, 0.0).astype(jnp.bfloat16)
    pick = jnp.concatenate([pick, pick], axis=0)

    high, low = split(src_ref[...])
    xh[0], xl[0] = high, low
    edge = jnp.zeros((rows, HB), jnp.bfloat16)
    for power in (1, 2):
        for buf in (xh, xl):
            buf[power, :, :HB] = edge
            buf[power, :, buf.shape[2] - HB :] = edge

    def build(b, _):
        at = pl.multiple_of(b * WB, WB)
        vh, vl = split(band_ref[:, pl.ds(at, WB)])
        both = jnp.concatenate([vh, vl], axis=0)
        diag = mm(both, pick, TN)
        band = pltpu.roll(diag, 0, 1, stride=1, stride_axis=0)
        wh[b], wl[b] = split(band)
        return 0

    lax.fori_loop(0, blocks, build, 0)

    def apply(power, b):
        at = pl.multiple_of(b * WB, WB)
        window = pl.ds(at, span)
        left_h = xh[power - 1, :, window]
        both = jnp.concatenate([left_h, xl[power - 1, :, window]], axis=0)
        by_high = mm(both, wh[b], NT)
        return by_high[:rows] + by_high[rows:] + mm(left_h, wl[b], NT)

    for power in (1, 2):

        def step(b, _):
            h, l = split(apply(power, b))
            place = pl.ds(pl.multiple_of(b * WB + HB, HB), WB)
            xh[power, :, place] = h
            xl[power, :, place] = l
            return 0

        lax.fori_loop(0, blocks, step, 0)

    for power in range(3):
        high_ref[power * rows : (power + 1) * rows, :] = xh[power, :, 3 * HB : 3 * HB + width]
        low_ref[power * rows : (power + 1) * rows, :] = xl[power, :, 3 * HB : 3 * HB + width]

    def last(b, acc):
        h, l = split(apply(3, b + 1))
        place = pl.ds(pl.multiple_of(b * WB, WB), WB)
        high_ref[3 * rows :, place] = h
        low_ref[3 * rows :, place] = l
        tall = high_ref[:, place]
        return acc + mm(tall, tall, NT) + 2.0 * mm(tall, low_ref[:, place], NT)

    gram = lax.fori_loop(0, blocks - 2, last, jnp.zeros((4 * rows, 4 * rows), jnp.float32))
    gram = (gram + gram.T) * (0.5 / total)
    half = gram.shape[1] // 2
    gram_ref[0] = gram[:, :half]
    gram_ref[1] = gram[:, half:]


def lane_copy(x, lane):
    return jnp.broadcast_to(x[:, lane : lane + 1], (8, 128))


def row_copy(x, row):
    return jnp.broadcast_to(x[row : row + 1, :], (8, 128))


def eliminate(work, tiles):
    order = work.shape[0]
    sub = lax.broadcasted_iota(jnp.int32, (8, 128), 0)

    def tile(g, t):
        return slice(8 * g, 8 * g + 8), slice(128 * t, 128 * t + 128)

    for kb in range(order // 8):
        own = [work[tile(kb, t)] for t in range(tiles)]
        cols = [lane_copy(own[0], 8 * kb + j) for j in range(8)]
        inverses, cross, tops = [], [], []
        pivots = jnp.ones((8, 128), jnp.float32)
        for k in range(8):
            pivot = row_copy(cols[k], k)
            inverse = 1.0 / pivot
            pivots = jnp.where(sub == k, pivot, pivots)
            m = jnp.where(sub > k, cols[k] * inverse, 0.0)
            crossing = [row_copy(cols[j], k) for j in range(k + 1, 8)]
            top = [row_copy(x, k) for x in own]
            for j in range(k + 1, 8):
                cols[j] = cols[j] - m * crossing[j - k - 1]
            own = [x - m * y for x, y in zip(own, top)]
            inverses.append(inverse)
            cross.append(crossing)
            tops.append(top)
        scale = lax.rsqrt(pivots)
        for t in range(1, tiles):
            work[tile(kb, t)] = own[t] * scale
        for g in range(kb + 1, order // 8):
            rest = [work[tile(g, t)] for t in range(tiles)]
            q = [lane_copy(rest[0], 8 * kb + j) for j in range(8)]
            for k in range(8):
                m = q[k] * inverses[k]
                for j in range(k + 1, 8):
                    q[j] = q[j] - m * cross[k][j - k - 1]
                rest = [x - m * y for x, y in zip(rest, tops[k])]
            for t in range(tiles):
                work[tile(g, t)] = rest[t]


def compress(gram, retain, work):
    order = gram.shape[0]
    spanning = gram[:retain]
    for turn in range(2):
        if turn > 0:
            spanning = exact(work[:, retain : retain + order], gram)
        mapped = exact(spanning, gram)
        metric = exact(mapped, spanning, NT)
        work[:, :retain] = 0.5 * (metric + metric.T)
        work[:, retain : retain + order] = spanning
        eliminate(work, (retain + order) // 128)
    return work[:, retain : retain + order]


def finish_kernel(gram_ref, high_ref, low_ref, out_ref, work):
    keep = out_ref.shape[0]
    g11 = gram_ref[0, :keep]
    g12 = gram_ref[1, :keep]
    g22 = gram_ref[1, keep:]
    one = compress(g11, keep, work)
    mixed = [exact(exact(one, g), one, NT) for g in (g11, g12, g22)]
    top = jnp.concatenate([mixed[0], mixed[1]], axis=1)
    bottom = jnp.concatenate([mixed[1].T, mixed[2]], axis=1)
    two = compress(jnp.concatenate([top, bottom], axis=0), keep, work)
    overall = jnp.concatenate([exact(two[:, :keep], one), exact(two[:, keep:], one)], axis=1)
    fh, fl = split(overall)
    both = jnp.concatenate([fh, fl], axis=0)

    def step(b, _):
        place = pl.ds(pl.multiple_of(b * WB, WB), WB)
        wide = mm(both, high_ref[:, place])
        out_ref[:, place] = wide[:keep] + wide[keep:] + mm(fh, low_ref[:, place])
        return 0

    lax.fori_loop(0, out_ref.shape[1] // WB, step, 0)


def body(source, band_values, offsets):
    devices = lax.axis_size("rows")
    rows, width = source.shape
    up = [(i, i + 1) for i in range(devices - 1)]
    down = [(i + 1, i) for i in range(devices - 1)]

    def extended(x, reach):
        low = lax.ppermute(x[:, width - reach :], "rows", up)
        high = lax.ppermute(x[:, :reach], "rows", down)
        return jnp.concatenate([low, x, high], axis=1)

    src = extended(source, 3 * HB)
    band = extended(band_values, 2 * HB)
    blocks = width // WB + 2
    wide = src.shape[1]
    high, low, gram = pl.pallas_call(
        functools.partial(powers_kernel, float(width * devices)),
        out_shape=[
            jax.ShapeDtypeStruct((4 * rows, width), jnp.bfloat16),
            jax.ShapeDtypeStruct((4 * rows, width), jnp.bfloat16),
            jax.ShapeDtypeStruct((2, 4 * rows, 2 * rows), jnp.float32),
        ],
        scratch_shapes=[
            pltpu.VMEM((3, rows, wide), jnp.bfloat16),
            pltpu.VMEM((3, rows, wide), jnp.bfloat16),
            pltpu.VMEM((blocks, WB, 2 * WB), jnp.bfloat16),
            pltpu.VMEM((blocks, WB, 2 * WB), jnp.bfloat16),
        ],
        compiler_params=pltpu.CompilerParams(vmem_limit_bytes=48 * 1024 * 1024),
        name="powers",
    )(src, band, offsets.reshape(-1, 1))

    parts = gram.reshape(devices, -1, 128)
    mine = lax.all_to_all(parts, "rows", 0, 0, tiled=True).sum(axis=0)
    copies = jnp.broadcast_to(mine, (devices, *mine.shape))
    gram = lax.all_to_all(copies, "rows", 0, 0, tiled=True).reshape(gram.shape)

    return pl.pallas_call(
        finish_kernel,
        out_shape=jax.ShapeDtypeStruct((2 * rows, width), jnp.float32),
        scratch_shapes=[pltpu.VMEM((2 * rows, 6 * rows), jnp.float32)],
        compiler_params=pltpu.CompilerParams(vmem_limit_bytes=48 * 1024 * 1024),
        name="finish",
    )(gram, high, low)


def solution(mesh):
    in_specs = (P(None, "rows"), P(None, "rows"), P())
    return jax.shard_map(
        body, mesh=mesh, in_specs=in_specs, out_specs=P(None, "rows"), check_vma=False
    )
```

```python
import functools

import jax
import jax.numpy as jnp
from jax import lax
from jax.experimental import pallas as pl
from jax.experimental.pallas import tpu as pltpu
from jax.sharding import Mesh
from jax.sharding import PartitionSpec as P

HB = 128
WB = 256
SPAN = 2 * WB
ROWS = ("far", "near")
NN = (((1,), (0,)), ((), ()))
NT = (((1,), (1,)), ((), ()))


def split(x):
    high = x.astype(jnp.bfloat16)
    return high, (x - high.astype(jnp.float32)).astype(jnp.bfloat16)


def mm(a, b, dims=NN):
    return lax.dot_general(a, b, dims, preferred_element_type=jnp.float32)


def exact(a, b, dims=NN):
    return lax.dot_general(
        a, b, dims, precision=lax.Precision.HIGHEST, preferred_element_type=jnp.float32
    )


def picker(off_ref):
    lanes = lax.broadcasted_iota(jnp.int32, (off_ref.shape[0], SPAN), 1)
    pick = jnp.where(lanes == off_ref[...] + HB, 1.0, 0.0).astype(jnp.bfloat16)
    return jnp.concatenate([pick, pick], axis=0)


def band_block(values, pick):
    diag = mm(jnp.concatenate(split(values.T), axis=1), pick)
    return split(pltpu.roll(diag, 0, 1, stride=1, stride_axis=0).T)


def blocks_kernel(band_ref, off_ref, wh, wl, pick_ref):
    pick_ref[...] = picker(off_ref)

    def build(b, _):
        at = pl.multiple_of(b * WB, WB)
        wh[b], wl[b] = band_block(band_ref[:, pl.ds(at, WB)], pick_ref[...])
        return 0

    lax.fori_loop(0, wh.shape[0], build, 0, unroll=2)


def powers_kernel(
    total, src_ref, low_in, high_in, off_ref, wh, wl, high_ref, low_ref, gram_ref, xs, eh, el
):
    rows, width = src_ref.shape
    inner = width // WB
    reach = 3 * HB
    edges = [(low_in, 0, 0), (high_in, 1, reach + width)]
    pick = picker(off_ref)
    for ref, side, at in edges:
        high, low = split(ref[:, :reach])
        xs[0, :rows, at : at + reach] = high
        xs[0, rows:, at : at + reach] = low
        values = jnp.concatenate([ref[:, reach : reach + WB], ref[:, reach + WB :]], axis=0)
        eh[side], el[side] = band_block(values, pick)

    def place(b, _):
        at = pl.multiple_of(b * WB, WB)
        high, low = split(src_ref[:, pl.ds(at, WB)])
        high_ref[:rows, pl.ds(at, WB)] = high
        low_ref[:rows, pl.ds(at, WB)] = low
        into = pl.ds(pl.multiple_of(b * WB + reach, HB), WB)
        xs[0, :rows, into] = high
        xs[0, rows:, into] = low
        return 0

    lax.fori_loop(0, inner, place, 0, unroll=2)
    for power in (1, 2):
        for at in (0, xs.shape[2] - HB):
            xs[power, :, at : at + HB] = jnp.zeros((2 * rows, HB), jnp.bfloat16)

    def apply(power, at, by_high, by_low):
        window = xs[power - 1, :, pl.ds(at, SPAN)]
        both = mm(window, by_high)
        return split(both[:rows] + both[rows:] + mm(window[:rows], by_low))

    def keep(power, at, pair):
        for part in range(2):
            xs[power, part * rows : (part + 1) * rows, pl.ds(at, WB)] = pair[part]

    for power in (1, 2, 3):
        if power < 3:
            for _, side, at in edges:
                at = at if side == 0 else at - HB
                keep(power, at + HB, apply(power, at, eh[side], el[side]))

        def step(b, _):
            at = pl.multiple_of(b * WB, WB)
            pair = apply(power, pl.multiple_of(at + WB, WB), wh[b], wl[b])
            high_ref[power * rows : (power + 1) * rows, pl.ds(at, WB)] = pair[0]
            low_ref[power * rows : (power + 1) * rows, pl.ds(at, WB)] = pair[1]
            if power < 3:
                keep(power, pl.multiple_of(at + reach, HB), pair)
            return 0

        lax.fori_loop(0, inner, step, 0, unroll=4)

    tall = high_ref[...]
    gram = mm(tall, tall, NT) + 2.0 * mm(tall, low_ref[...], NT)
    pack(gram_ref, (gram + gram.T) * (0.5 / total))


def places(order):
    shape = (order, order)
    down = lax.broadcasted_iota(jnp.int32, shape, 0)
    return lax.broadcasted_iota(jnp.int32, shape, 1) - down


def pack(ref, gram):
    half = ref.shape[2]
    part = half // ref.shape[0]
    across = places(half)
    tail = gram[half:, half:]
    ref[:, :part] = gram[:half, half:].reshape(-1, part, half)
    both = jnp.where(across >= 0, gram[:half, :half], tail)
    ref[:, part : 2 * part] = both.reshape(-1, part, half)
    ref[:, 2 * part :] = jnp.zeros((ref.shape[0], 8, half), jnp.float32)
    middle = jnp.sum(jnp.where(across == 0, tail, 0.0), axis=0, keepdims=True)
    ref[0, 2 * part : 2 * part + 1] = middle


def unpack(ref):
    half = ref.shape[2]
    part = half // ref.shape[0]
    across = places(half)
    cross = ref[:, :part].reshape(half, half)
    both = ref[:, part : 2 * part].reshape(half, half)
    middle = jnp.broadcast_to(ref[0, 2 * part : 2 * part + 1], (half, half))
    upper = jnp.where(across > 0, both, 0.0)
    lower = jnp.where(across < 0, both, 0.0)
    head = upper + upper.T + jnp.where(across == 0, both, 0.0)
    tail = lower + lower.T + jnp.where(across == 0, middle, 0.0)
    return head, cross, tail


def lane_copy(x, lane):
    return jnp.broadcast_to(x[:, lane : lane + 1], (8, 128))


def row_copy(x, row):
    return jnp.broadcast_to(x[row : row + 1, :], (8, 128))


def eliminate(work, tiles):
    order = work.shape[0]
    sub = lax.broadcasted_iota(jnp.int32, (8, 128), 0)

    def tile(g, t):
        return slice(8 * g, 8 * g + 8), slice(128 * t, 128 * t + 128)

    for kb in range(order // 8):
        own = [work[tile(kb, t)] for t in range(tiles)]
        cols = [lane_copy(own[0], 8 * kb + j) for j in range(8)]
        inverses, cross, tops = [], [], []
        pivots = jnp.ones((8, 128), jnp.float32)
        for k in range(8):
            pivot = row_copy(cols[k], k)
            inverse = 1.0 / pivot
            pivots = jnp.where(sub == k, pivot, pivots)
            m = jnp.where(sub > k, cols[k] * inverse, 0.0)
            crossing = [row_copy(cols[j], k) for j in range(k + 1, 8)]
            top = [row_copy(x, k) for x in own]
            for j in range(k + 1, 8):
                cols[j] = cols[j] - m * crossing[j - k - 1]
            own = [x - m * y for x, y in zip(own, top)]
            inverses.append(inverse)
            cross.append(crossing)
            tops.append(top)
        scale = lax.rsqrt(pivots)
        for t in range(1, tiles):
            work[tile(kb, t)] = own[t] * scale
        for g in range(kb + 1, order // 8):
            rest = [work[tile(g, t)] for t in range(tiles)]
            q = [lane_copy(rest[0], 8 * kb + j) for j in range(8)]
            for k in range(8):
                m = q[k] * inverses[k]
                for j in range(k + 1, 8):
                    q[j] = q[j] - m * cross[k][j - k - 1]
                rest = [x - m * y for x, y in zip(rest, tops[k])]
            for t in range(tiles):
                work[tile(g, t)] = rest[t]


def compress(gram, retain, work):
    order = gram.shape[0]
    spanning = gram[:retain]
    for turn in range(2):
        if turn > 0:
            spanning = exact(work[:, retain : retain + order], gram)
        mapped = exact(spanning, gram)
        metric = exact(mapped, spanning, NT)
        work[:, :retain] = 0.5 * (metric + metric.T)
        work[:, retain : retain + order] = spanning
        eliminate(work, (retain + order) // 128)
    return work[:, retain : retain + order]


def finish_kernel(gram_ref, high_ref, low_ref, out_ref, work):
    keep = out_ref.shape[0]
    g11, g12, g22 = unpack(gram_ref)
    one = compress(g11, keep, work)
    mixed = [exact(exact(one, g), one, NT) for g in (g11, g12, g22)]
    top = jnp.concatenate([mixed[0], mixed[1]], axis=1)
    bottom = jnp.concatenate([mixed[1].T, mixed[2]], axis=1)
    two = compress(jnp.concatenate([top, bottom], axis=0), keep, work)
    overall = jnp.concatenate([exact(two[:, :keep], one), exact(two[:, keep:], one)], axis=1)
    fh, fl = split(overall)
    both = jnp.concatenate([fh, fl], axis=0)

    def step(b, _):
        place = pl.ds(pl.multiple_of(b * WB, WB), WB)
        wide = mm(both, high_ref[:, place])
        out_ref[:, place] = wide[:keep] + wide[keep:] + mm(fh, low_ref[:, place])
        return 0

    lax.fori_loop(0, out_ref.shape[1] // WB, step, 0)


def exchange(blocks, axis):
    return lax.all_to_all(blocks, axis, 0, 0, tiled=True)


def copies(x, axis):
    return exchange(jnp.broadcast_to(x, (lax.axis_size(axis), *x.shape)), axis)


def body(source, band_values, offsets):
    devices = lax.axis_size(ROWS)
    group = lax.axis_size("near")
    rows, width = source.shape
    reach = 3 * HB
    inner = width // WB
    up = [(i, i + 1) for i in range(devices - 1)]
    down = [(i + 1, i) for i in range(devices - 1)]

    def packed(far, near):
        return jnp.concatenate([far, near[:rows], near[rows:]], axis=1)

    low = lax.ppermute(packed(source[:, width - reach :], band_values[:, width - WB :]), ROWS, up)
    high = lax.ppermute(packed(source[:, :reach], band_values[:, :WB]), ROWS, down)
    offsets = offsets.reshape(-1, 1)
    blocks = jax.ShapeDtypeStruct((inner, SPAN, WB), jnp.bfloat16)
    by_high, by_low = pl.pallas_call(
        blocks_kernel,
        out_shape=[blocks, blocks],
        scratch_shapes=[pltpu.VMEM((2 * HB, SPAN), jnp.bfloat16)],
        compiler_params=pltpu.CompilerParams(vmem_limit_bytes=12 * 1024 * 1024),
        cost_estimate=pl.CostEstimate(
            flops=10_000_000_000, bytes_accessed=12_000_000, transcendentals=0
        ),
        name="blocks",
    )(band_values, offsets)
    wide = width + 2 * reach
    high, low, gram = pl.pallas_call(
        functools.partial(powers_kernel, float(width * devices)),
        out_shape=[
            jax.ShapeDtypeStruct((4 * rows, width), jnp.bfloat16),
            jax.ShapeDtypeStruct((4 * rows, width), jnp.bfloat16),
            jax.ShapeDtypeStruct((group, 4 * rows // group + 8, 2 * rows), jnp.float32),
        ],
        scratch_shapes=[
            pltpu.VMEM((3, 2 * rows, wide), jnp.bfloat16),
            pltpu.VMEM((2, SPAN, WB), jnp.bfloat16),
            pltpu.VMEM((2, SPAN, WB), jnp.bfloat16),
        ],
        compiler_params=pltpu.CompilerParams(vmem_limit_bytes=16 * 1024 * 1024),
        name="powers",
    )(source, low, high, offsets, by_high, by_low)

    gram = exchange(gram, "near").sum(axis=0)
    gram = copies(gram, "far").sum(axis=0)
    gram = copies(gram, "near")

    return pl.pallas_call(
        finish_kernel,
        out_shape=jax.ShapeDtypeStruct((2 * rows, width), jnp.float32),
        scratch_shapes=[pltpu.VMEM((2 * rows, 6 * rows), jnp.float32)],
        compiler_params=pltpu.CompilerParams(vmem_limit_bytes=16 * 1024 * 1024),
        name="finish",
    )(gram, high, low)


def solution(mesh):
    devices = mesh.devices.size
    near = 1 << (devices.bit_length() // 2)
    grid = Mesh(mesh.devices.reshape(devices // near, near), ROWS)
    split_rows = P(None, ROWS)
    return jax.shard_map(
        body,
        mesh=grid,
        in_specs=(split_rows, split_rows, P()),
        out_specs=split_rows,
        check_vma=False,
    )
```

```python
import functools

import jax
import jax.numpy as jnp
from jax import lax
from jax.experimental import pallas as pl
from jax.experimental.pallas import tpu as pltpu
from jax.sharding import Mesh
from jax.sharding import PartitionSpec as P

HB = 128
WB = 256
SPAN = 2 * WB
ROWS = ("far", "near")
NN = (((1,), (0,)), ((), ()))
NT = (((1,), (1,)), ((), ()))


def split(x):
    high = x.astype(jnp.bfloat16)
    return high, (x - high.astype(jnp.float32)).astype(jnp.bfloat16)


def mm(a, b, dims=NN):
    return lax.dot_general(a, b, dims, preferred_element_type=jnp.float32)


def exact(a, b, dims=NN):
    return lax.dot_general(
        a, b, dims, precision=lax.Precision.HIGHEST, preferred_element_type=jnp.float32
    )


def picker(off_ref):
    lanes = lax.broadcasted_iota(jnp.int32, (off_ref.shape[0], 3 * HB), 1)
    pick = jnp.where(lanes == off_ref[...] + HB, 1.0, 0.0).astype(jnp.bfloat16)
    return jnp.concatenate([pick, pick], axis=0)


def diagonals(values, pick):
    return mm(jnp.concatenate(split(values.T), axis=1), pick)


def place_block(diag, wh, wl, b):
    for half in range(2):
        rows = slice(half * HB, half * HB + HB)
        band = pltpu.roll(diag[rows], 0, 1, stride=1, stride_axis=0)
        high, low = split(band.T)
        for ref, part in ((wh, high), (wl, low)):
            ref[b, half * HB : half * HB + 3 * HB, rows] = part
            empty = 3 * HB * (1 - half)
            ref[b, empty : empty + HB, rows] = jnp.zeros((HB, HB), jnp.bfloat16)


def blocks_kernel(band_ref, off_ref, wh, wl, diag_ref):
    pick = picker(off_ref)
    count = wh.shape[0]
    for b in range(count + 1):
        if b < count:
            diag_ref[b % 2] = diagonals(band_ref[:, b * WB : b * WB + WB], pick)
        if b > 0:
            place_block(diag_ref[(b - 1) % 2], wh, wl, b - 1)


def powers_kernel(
    total, src_ref, low_in, high_in, off_ref, wh, wl, high_ref, low_ref, gram_ref, xs, eh, el
):
    rows, width = src_ref.shape
    inner = width // WB
    reach = 3 * HB
    edges = [(low_in, 0, 0), (high_in, 1, reach + width)]
    for b in range(inner):
        at = slice(b * WB, b * WB + WB)
        into = slice(b * WB + reach, b * WB + reach + WB)
        high, low = split(src_ref[:, at])
        high_ref[:rows, at] = high
        low_ref[:rows, at] = low
        xs[0, :rows, into] = high
        xs[0, rows:, into] = low
    pick = picker(off_ref)
    for ref, side, at in edges:
        high, low = split(ref[:, :reach])
        xs[0, :rows, at : at + reach] = high
        xs[0, rows:, at : at + reach] = low
        values = jnp.concatenate([ref[:, reach : reach + WB], ref[:, reach + WB :]], axis=0)
        place_block(diagonals(values, pick), eh, el, side)
    for power in (1, 2):
        for at in (0, xs.shape[2] - HB):
            xs[power, :, at : at + HB] = jnp.zeros((2 * rows, HB), jnp.bfloat16)

    def apply(power, at, by_high, by_low):
        window = xs[power - 1, :, at : at + SPAN]
        both = mm(window, by_high)
        return split(both[:rows] + both[rows:] + mm(window[:rows], by_low))

    for power in (1, 2, 3):
        inside = list(range(2, inner)) + [1, inner]
        for b in inside + [0, inner + 1] * (power < 3):
            if b in (0, inner + 1):
                by = (eh[int(b > 0)], el[int(b > 0)])
            else:
                by = (wh[b - 1], wl[b - 1])
            pair = apply(power, b * WB, *by)
            if power < 3:
                for part in range(2):
                    place = slice(b * WB + HB, b * WB + HB + WB)
                    xs[power, part * rows : (part + 1) * rows, place] = pair[part]
            if 0 < b <= inner:
                for ref, value in zip((high_ref, low_ref), pair):
                    ref[power * rows : (power + 1) * rows, b * WB - WB : b * WB] = value

    tall = high_ref[...]
    gram = mm(tall, tall, NT) + 2.0 * mm(tall, low_ref[...], NT)
    pack(gram_ref, (gram + gram.T) * (0.5 / total))


def places(order):
    shape = (order, order)
    down = lax.broadcasted_iota(jnp.int32, shape, 0)
    return lax.broadcasted_iota(jnp.int32, shape, 1) - down


def pack(ref, gram):
    half = ref.shape[1]
    across = places(half)
    tail = gram[half:, half:]
    ref[:half] = gram[:half, half:]
    ref[half : 2 * half] = jnp.where(across >= 0, gram[:half, :half], tail)
    ref[2 * half :] = jnp.zeros((ref.shape[0] - 2 * half, half), jnp.float32)
    middle = jnp.sum(jnp.where(across == 0, tail, 0.0), axis=0, keepdims=True)
    ref[2 * half : 2 * half + 1] = middle


def unpack(ref):
    half = ref.shape[1]
    across = places(half)
    cross = ref[:half]
    both = ref[half : 2 * half]
    middle = jnp.broadcast_to(ref[2 * half : 2 * half + 1], (half, half))
    upper = jnp.where(across > 0, both, 0.0)
    lower = jnp.where(across < 0, both, 0.0)
    head = upper + upper.T + jnp.where(across == 0, both, 0.0)
    tail = lower + lower.T + jnp.where(across == 0, middle, 0.0)
    return head, cross, tail


def lane_copy(x, lane):
    return jnp.broadcast_to(x[:, lane : lane + 1], (8, 128))


def row_copy(x, row):
    return jnp.broadcast_to(x[row : row + 1, :], (8, 128))


def eliminate(work, tiles):
    order = work.shape[0]
    sub = lax.broadcasted_iota(jnp.int32, (8, 128), 0)

    def tile(g, t):
        return slice(8 * g, 8 * g + 8), slice(128 * t, 128 * t + 128)

    for kb in range(order // 8):
        own = [work[tile(kb, t)] for t in range(tiles)]
        cols = [lane_copy(own[0], 8 * kb + j) for j in range(8)]
        inverses, cross, tops = [], [], []
        pivots = jnp.ones((8, 128), jnp.float32)
        for k in range(8):
            pivot = row_copy(cols[k], k)
            inverse = 1.0 / pivot
            pivots = jnp.where(sub == k, pivot, pivots)
            m = jnp.where(sub > k, cols[k] * inverse, 0.0)
            crossing = [row_copy(cols[j], k) for j in range(k + 1, 8)]
            top = [row_copy(x, k) for x in own]
            for j in range(k + 1, 8):
                cols[j] = cols[j] - m * crossing[j - k - 1]
            own = [x - m * y for x, y in zip(own, top)]
            inverses.append(inverse)
            cross.append(crossing)
            tops.append(top)
        scale = lax.rsqrt(pivots)
        for t in range(1, tiles):
            work[tile(kb, t)] = own[t] * scale
        for g in range(kb + 1, order // 8):
            rest = [work[tile(g, t)] for t in range(tiles)]
            q = [lane_copy(rest[0], 8 * kb + j) for j in range(8)]
            for k in range(8):
                m = q[k] * inverses[k]
                for j in range(k + 1, 8):
                    q[j] = q[j] - m * cross[k][j - k - 1]
                rest = [x - m * y for x, y in zip(rest, tops[k])]
            for t in range(tiles):
                work[tile(g, t)] = rest[t]


def compress(gram, retain, work):
    order = gram.shape[0]
    spanning = gram[:retain]
    for turn in range(2):
        if turn > 0:
            spanning = exact(work[:, retain : retain + order], gram)
        mapped = exact(spanning, gram)
        metric = exact(mapped, spanning, NT)
        work[:, :retain] = 0.5 * (metric + metric.T)
        work[:, retain : retain + order] = spanning
        eliminate(work, (retain + order) // 128)
    return work[:, retain : retain + order]


def finish_kernel(gram_ref, high_ref, low_ref, out_ref, work):
    keep = out_ref.shape[0]
    g11, g12, g22 = unpack(gram_ref)
    one = compress(g11, keep, work)
    cross = exact(exact(one, g12), one, NT)
    tail = exact(exact(one, g22), one, NT)
    same = jnp.where(places(keep) == 0, 1.0, 0.0)
    top = jnp.concatenate([same, cross], axis=1)
    bottom = jnp.concatenate([cross.T, tail], axis=1)
    two = compress(jnp.concatenate([top, bottom], axis=0), keep, work)
    overall = jnp.concatenate([exact(two[:, :keep], one), exact(two[:, keep:], one)], axis=1)
    fh, fl = split(overall)
    both = jnp.concatenate([fh, fl], axis=0)

    for b in range(out_ref.shape[1] // WB):
        place = slice(b * WB, b * WB + WB)
        wide = mm(both, high_ref[:, place])
        out_ref[:, place] = wide[:keep] + wide[keep:] + mm(fh, low_ref[:, place])


def exchange(blocks, axis):
    return lax.all_to_all(blocks, axis, 0, 0, tiled=True)


def copies(x, axis):
    return exchange(jnp.broadcast_to(x, (lax.axis_size(axis), *x.shape)), axis)


def body(source, band_values, offsets):
    devices = lax.axis_size(ROWS)
    group = lax.axis_size("near")
    rows, width = source.shape
    reach = 3 * HB
    inner = width // WB
    up = [(i, i + 1) for i in range(devices - 1)]
    down = [(i + 1, i) for i in range(devices - 1)]

    def packed(far, near):
        return jnp.concatenate([far, near[:rows], near[rows:]], axis=1)

    low = lax.ppermute(packed(source[:, width - reach :], band_values[:, width - WB :]), ROWS, up)
    high = lax.ppermute(packed(source[:, :reach], band_values[:, :WB]), ROWS, down)
    offsets = offsets.reshape(-1, 1)
    blocks = jax.ShapeDtypeStruct((inner, SPAN, WB), jnp.bfloat16)
    by_high, by_low = pl.pallas_call(
        blocks_kernel,
        out_shape=[blocks, blocks],
        scratch_shapes=[pltpu.VMEM((2, WB, 3 * HB), jnp.float32)],
        compiler_params=pltpu.CompilerParams(vmem_limit_bytes=12 * 1024 * 1024),
        cost_estimate=pl.CostEstimate(
            flops=10_000_000_000, bytes_accessed=12_000_000, transcendentals=0
        ),
        name="blocks",
    )(band_values, offsets)
    wide = width + 2 * reach
    high, low, gram = pl.pallas_call(
        functools.partial(powers_kernel, float(width * devices)),
        out_shape=[
            jax.ShapeDtypeStruct((4 * rows, width), jnp.bfloat16),
            jax.ShapeDtypeStruct((4 * rows, width), jnp.bfloat16),
            jax.ShapeDtypeStruct((4 * rows + 16, 2 * rows), jnp.float32),
        ],
        scratch_shapes=[
            pltpu.VMEM((3, 2 * rows, wide), jnp.bfloat16),
            pltpu.VMEM((2, SPAN, WB), jnp.bfloat16),
            pltpu.VMEM((2, SPAN, WB), jnp.bfloat16),
        ],
        compiler_params=pltpu.CompilerParams(vmem_limit_bytes=16 * 1024 * 1024),
        name="powers",
    )(source, low, high, offsets, by_high, by_low)

    gram = exchange(gram.reshape(group, -1, 1, 2 * rows), "near").sum(axis=0)
    gram = copies(gram, "far").sum(axis=0)
    gram = copies(gram, "near").reshape(4 * rows + 16, 2 * rows)

    return pl.pallas_call(
        finish_kernel,
        out_shape=jax.ShapeDtypeStruct((2 * rows, width), jnp.float32),
        scratch_shapes=[pltpu.VMEM((2 * rows, 6 * rows), jnp.float32)],
        compiler_params=pltpu.CompilerParams(vmem_limit_bytes=16 * 1024 * 1024),
        name="finish",
    )(gram, high, low)


def solution(mesh):
    devices = mesh.devices.size
    near = 1 << (devices.bit_length() // 2)
    grid = Mesh(mesh.devices.reshape(devices // near, near), ROWS)
    split_rows = P(None, ROWS)
    return jax.shard_map(
        body,
        mesh=grid,
        in_specs=(split_rows, split_rows, P()),
        out_specs=split_rows,
        check_vma=False,
    )
```

```python
import functools

import jax
import jax.numpy as jnp
from jax import lax
from jax.experimental import pallas as pl
from jax.experimental.pallas import tpu as pltpu
from jax.sharding import Mesh
from jax.sharding import PartitionSpec as P

HB = 128
WB = 256
SPAN = 2 * WB
ROWS = ("far", "near")
NN = (((1,), (0,)), ((), ()))
NT = (((1,), (1,)), ((), ()))


def split(x):
    high = x.astype(jnp.bfloat16)
    return high, (x - high.astype(jnp.float32)).astype(jnp.bfloat16)


def mm(a, b, dims=NN):
    return lax.dot_general(a, b, dims, preferred_element_type=jnp.float32)


def exact(a, b, dims=NN):
    return lax.dot_general(
        a, b, dims, precision=lax.Precision.HIGHEST, preferred_element_type=jnp.float32
    )


def picker(off_ref):
    down = lax.broadcasted_iota(jnp.int32, (3 * HB, off_ref.shape[1]), 0)
    pick = jnp.where(down == off_ref[...] + HB, 1.0, 0.0).astype(jnp.bfloat16)
    return jnp.concatenate([pick, pick], axis=1)


def diagonals(values, pick):
    return mm(jnp.concatenate(split(values.T), axis=1), pick, NT)


def place_block(diag, wh, wl, b):
    for half in range(2):
        rows = slice(half * HB, half * HB + HB)
        band = pltpu.roll(diag[rows], 0, 1, stride=1, stride_axis=0)
        high, low = split(band.T)
        for ref, part in ((wh, high), (wl, low)):
            ref[b, half * HB : half * HB + 3 * HB, rows] = part
            empty = 3 * HB * (1 - half)
            ref[b, empty : empty + HB, rows] = jnp.zeros((HB, HB), jnp.bfloat16)


def blocks_kernel(band_ref, off_ref, wh, wl, diag_ref):
    pick = picker(off_ref)
    count = wh.shape[0]
    for b in range(count + 1):
        if b < count:
            diag_ref[b % 2] = diagonals(band_ref[:, b * WB : b * WB + WB], pick)
        if b > 0:
            place_block(diag_ref[(b - 1) % 2], wh, wl, b - 1)


def edges_kernel(src_ref, band_ref, up_ref, down_ref, sems):
    rows, width = src_ref.shape
    reach = 3 * HB
    copies = []
    for ref, far, near in ((up_ref, width - reach, width - WB), (down_ref, 0, 0)):
        parts = [(src_ref.at[:, pl.ds(far, reach)], ref.at[:, pl.ds(0, reach)])]
        for half in range(2):
            take = band_ref.at[pl.ds(half * rows, rows), pl.ds(near, WB)]
            parts.append((take, ref.at[:, pl.ds(reach + half * WB, WB)]))
        for one, two in parts:
            copies.append(pltpu.make_async_copy(one, two, sems.at[len(copies)]))
    for copy in copies:
        copy.start()
    for copy in copies:
        copy.wait()


def powers_kernel(
    total, src_ref, low_in, high_in, off_ref, wh, wl, high_ref, low_ref, gram_ref, xs, eh, el
):
    rows, width = src_ref.shape
    inner = width // WB
    reach = 3 * HB
    edges = [(low_in, 0, 0), (high_in, 1, reach + width)]
    for b in range(inner):
        at = slice(b * WB, b * WB + WB)
        into = slice(b * WB + reach, b * WB + reach + WB)
        high, low = split(src_ref[:, at])
        high_ref[:rows, at] = high
        low_ref[:rows, at] = low
        xs[0, :rows, into] = high
        xs[0, rows:, into] = low
    pick = picker(off_ref)
    for ref, side, at in edges:
        high, low = split(ref[:, :reach])
        xs[0, :rows, at : at + reach] = high
        xs[0, rows:, at : at + reach] = low
        values = jnp.concatenate([ref[:, reach : reach + WB], ref[:, reach + WB :]], axis=0)
        place_block(diagonals(values, pick), eh, el, side)
    for power in (1, 2):
        for at in (0, xs.shape[2] - HB):
            xs[power, :, at : at + HB] = jnp.zeros((2 * rows, HB), jnp.bfloat16)

    def apply(power, at, by_high, by_low):
        window = xs[power - 1, :, at : at + SPAN]
        both = mm(window, by_high)
        return split(both[:rows] + both[rows:] + mm(window[:rows], by_low))

    for power in (1, 2, 3):
        inside = list(range(2, inner)) + [1, inner]
        for b in inside + [0, inner + 1] * (power < 3):
            if b in (0, inner + 1):
                by = (eh[int(b > 0)], el[int(b > 0)])
            else:
                by = (wh[b - 1], wl[b - 1])
            pair = apply(power, b * WB, *by)
            if power < 3:
                for part in range(2):
                    place = slice(b * WB + HB, b * WB + HB + WB)
                    xs[power, part * rows : (part + 1) * rows, place] = pair[part]
            if 0 < b <= inner:
                for ref, value in zip((high_ref, low_ref), pair):
                    ref[power * rows : (power + 1) * rows, b * WB - WB : b * WB] = value
    tall = high_ref[...]
    gram = mm(tall, tall, NT) + 2.0 * mm(tall, low_ref[...], NT)
    pack(gram_ref, (gram + gram.T) * (0.5 / total))


def places(order):
    shape = (order, order)
    down = lax.broadcasted_iota(jnp.int32, shape, 0)
    return lax.broadcasted_iota(jnp.int32, shape, 1) - down


def pack(ref, gram):
    half = ref.shape[1]
    across = places(half)
    tail = gram[half:, half:]
    ref[:half] = gram[:half, half:]
    ref[half : 2 * half] = jnp.where(across >= 0, gram[:half, :half], tail)
    ref[2 * half :] = jnp.zeros((ref.shape[0] - 2 * half, half), jnp.float32)
    middle = jnp.sum(jnp.where(across == 0, tail, 0.0), axis=0, keepdims=True)
    ref[2 * half : 2 * half + 1] = middle


def unpack(ref):
    half = ref.shape[1]
    across = places(half)
    cross = ref[:half]
    both = ref[half : 2 * half]
    middle = jnp.broadcast_to(ref[2 * half : 2 * half + 1], (half, half))
    upper = jnp.where(across > 0, both, 0.0)
    lower = jnp.where(across < 0, both, 0.0)
    head = upper + upper.T + jnp.where(across == 0, both, 0.0)
    tail = lower + lower.T + jnp.where(across == 0, middle, 0.0)
    return head, cross, tail


def lane_copy(x, lane):
    return jnp.broadcast_to(x[:, lane : lane + 1], (8, 128))


def row_copy(x, row):
    return jnp.broadcast_to(x[row : row + 1, :], (8, 128))


def eliminate(work, tiles):
    order = work.shape[0]
    sub = lax.broadcasted_iota(jnp.int32, (8, 128), 0)

    def tile(g, t):
        return slice(8 * g, 8 * g + 8), slice(128 * t, 128 * t + 128)

    for kb in range(order // 8):
        own = [work[tile(kb, t)] for t in range(tiles)]
        cols = [lane_copy(own[0], 8 * kb + j) for j in range(8)]
        inverses, cross, tops = [], [], []
        pivots = jnp.ones((8, 128), jnp.float32)
        for k in range(8):
            pivot = row_copy(cols[k], k)
            inverse = 1.0 / pivot
            pivots = jnp.where(sub == k, pivot, pivots)
            m = jnp.where(sub > k, cols[k] * inverse, 0.0)
            crossing = [row_copy(cols[j], k) for j in range(k + 1, 8)]
            top = [row_copy(x, k) for x in own]
            for j in range(k + 1, 8):
                cols[j] = cols[j] - m * crossing[j - k - 1]
            own = [x - m * y for x, y in zip(own, top)]
            inverses.append(inverse)
            cross.append(crossing)
            tops.append(top)
        scale = lax.rsqrt(pivots)
        for t in range(1, tiles):
            work[tile(kb, t)] = own[t] * scale
        for g in range(kb + 1, order // 8):
            rest = [work[tile(g, t)] for t in range(tiles)]
            q = [lane_copy(rest[0], 8 * kb + j) for j in range(8)]
            for k in range(8):
                m = q[k] * inverses[k]
                for j in range(k + 1, 8):
                    q[j] = q[j] - m * cross[k][j - k - 1]
                rest = [x - m * y for x, y in zip(rest, tops[k])]
            for t in range(tiles):
                work[tile(g, t)] = rest[t]


def compress(gram, spanning, work):
    retain, order = spanning.shape
    metric = exact(exact(spanning, gram), spanning, NT)
    work[:, :retain] = 0.5 * (metric + metric.T)
    work[:, retain : retain + order] = spanning
    eliminate(work, (retain + order) // 128)
    return work[:, retain : retain + order]


def finish_kernel(gram_ref, high_ref, low_ref, out_ref, work, out, sems):
    keep = out_ref.shape[0]
    g11, g12, g22 = unpack(gram_ref)
    one = compress(g11, g11, work)
    one = compress(g11, exact(one, g11), work)
    cross = exact(exact(one, g12), one, NT)
    tail = exact(exact(one, g22), one, NT)
    same = jnp.where(places(keep) == 0, 1.0, 0.0)
    top = jnp.concatenate([same, cross], axis=1)
    bottom = jnp.concatenate([cross.T, tail], axis=1)
    gram = jnp.concatenate([top, bottom], axis=0)
    two = compress(gram, exact(top, gram), work)
    overall = jnp.concatenate([exact(two[:, :keep], one), exact(two[:, keep:], one)], axis=1)
    fh, fl = split(overall)
    both = jnp.concatenate([fh, fl], axis=0)

    quarter = out.shape[1] // 4
    stores = []
    for b in range(out.shape[1] // WB):
        place = slice(b * WB, b * WB + WB)
        wide = mm(both, high_ref[:, place])
        out[:, place] = wide[:keep] + wide[keep:] + mm(fh, low_ref[:, place])
        if (b + 1) * WB % quarter == 0:
            at = pl.ds((b + 1) * WB - quarter, quarter)
            sem = sems.at[len(stores)]
            stores.append(pltpu.make_async_copy(out.at[:, at], out_ref.at[:, at], sem))
            stores[-1].start()
    for store in stores:
        store.wait()


def sum_kernel(in_ref, out_ref):
    total = in_ref[0]
    for i in range(1, in_ref.shape[0]):
        total = total + in_ref[i]
    for i in range(out_ref.shape[0]):
        out_ref[i] = total


def exchange(blocks, axis):
    return lax.all_to_all(blocks, axis, 0, 0, tiled=True)


def summed_copies(blocks, axis):
    copies = pl.pallas_call(
        sum_kernel,
        out_shape=jax.ShapeDtypeStruct((lax.axis_size(axis), *blocks.shape[1:]), jnp.float32),
        compiler_params=pltpu.CompilerParams(vmem_limit_bytes=8 * 1024 * 1024),
        name="sums_" + axis,
    )(blocks)
    return exchange(copies, axis)


def body(source, band_values, offsets):
    devices = lax.axis_size(ROWS)
    group = lax.axis_size("near")
    rows, width = source.shape
    reach = 3 * HB
    inner = width // WB
    up = [(i, i + 1) for i in range(devices - 1)]
    down = [(i + 1, i) for i in range(devices - 1)]

    hbm = pl.BlockSpec(memory_space=pltpu.HBM)
    vmem = pl.BlockSpec(memory_space=pltpu.VMEM)
    edge = jax.ShapeDtypeStruct((rows, reach + 2 * WB), jnp.float32)
    last, first = pl.pallas_call(
        edges_kernel,
        out_shape=[edge, edge],
        in_specs=[hbm, hbm],
        scratch_shapes=[pltpu.SemaphoreType.DMA((6,))],
        compiler_params=pltpu.CompilerParams(vmem_limit_bytes=64_500_000),
        name="edges",
    )(source, band_values)
    low = lax.ppermute(last, ROWS, up)
    high = lax.ppermute(first, ROWS, down)
    offsets = offsets.reshape(1, -1)
    blocks = jax.ShapeDtypeStruct((inner, SPAN, WB), jnp.bfloat16)
    by_high, by_low = pl.pallas_call(
        blocks_kernel,
        out_shape=[blocks, blocks],
        scratch_shapes=[pltpu.VMEM((2, WB, 3 * HB), jnp.float32)],
        compiler_params=pltpu.CompilerParams(vmem_limit_bytes=12 * 1024 * 1024),
        cost_estimate=pl.CostEstimate(
            flops=10_000_000_000, bytes_accessed=12_000_000, transcendentals=0
        ),
        name="blocks",
    )(band_values, offsets)
    wide = width + 2 * reach
    high, low, gram = pl.pallas_call(
        functools.partial(powers_kernel, float(width * devices)),
        out_shape=[
            jax.ShapeDtypeStruct((4 * rows, width), jnp.bfloat16),
            jax.ShapeDtypeStruct((4 * rows, width), jnp.bfloat16),
            jax.ShapeDtypeStruct((4 * rows + 16, 2 * rows), jnp.float32),
        ],
        scratch_shapes=[
            pltpu.VMEM((3, 2 * rows, wide), jnp.bfloat16),
            pltpu.VMEM((2, SPAN, WB), jnp.bfloat16),
            pltpu.VMEM((2, SPAN, WB), jnp.bfloat16),
        ],
        compiler_params=pltpu.CompilerParams(vmem_limit_bytes=16 * 1024 * 1024),
        name="powers",
    )(source, low, high, offsets, by_high, by_low)

    gram = exchange(gram.reshape(group, -1, 1, 2 * rows), "near")
    gram = summed_copies(summed_copies(gram, "far"), "near")
    gram = gram.reshape(4 * rows + 16, 2 * rows)

    return pl.pallas_call(
        finish_kernel,
        out_shape=jax.ShapeDtypeStruct((2 * rows, width), jnp.float32),
        out_specs=hbm,
        scratch_shapes=[
            pltpu.VMEM((2 * rows, 6 * rows), jnp.float32),
            pltpu.VMEM((2 * rows, width), jnp.float32),
            pltpu.SemaphoreType.DMA((4,)),
        ],
        compiler_params=pltpu.CompilerParams(vmem_limit_bytes=16 * 1024 * 1024),
        name="finish",
    )(gram, high, low)


def solution(mesh):
    devices = mesh.devices.size
    near = 1 << (devices.bit_length() // 2)
    grid = Mesh(mesh.devices.reshape(devices // near, near), ROWS)
    split_rows = P(None, ROWS)
    return jax.shard_map(
        body,
        mesh=grid,
        in_specs=(split_rows, split_rows, P()),
        out_specs=split_rows,
        check_vma=False,
    )
```

```python
import functools

import jax
import jax.numpy as jnp
from jax import lax
from jax.experimental import pallas as pl
from jax.experimental.pallas import tpu as pltpu
from jax.sharding import Mesh
from jax.sharding import PartitionSpec as P

HB = 128
WB = 256
SPAN = 2 * WB
ROWS = ("far", "near")
NN = (((1,), (0,)), ((), ()))
NT = (((1,), (1,)), ((), ()))


def split(x):
    high = x.astype(jnp.bfloat16)
    return high, (x - high.astype(jnp.float32)).astype(jnp.bfloat16)


def mm(a, b, dims=NN):
    return lax.dot_general(a, b, dims, preferred_element_type=jnp.float32)


def exact(a, b, dims=NN):
    return lax.dot_general(
        a, b, dims, precision=lax.Precision.HIGHEST, preferred_element_type=jnp.float32
    )


def picker(off_ref):
    count = off_ref.shape[1]
    down = lax.broadcasted_iota(jnp.int32, (2 * HB, count), 0)
    pick = jnp.where(down == off_ref[...] + HB, 1.0, 0.0).astype(jnp.bfloat16)
    last = jnp.where(off_ref[...] == HB, 1.0, 0.0)
    last = jnp.sum(jnp.where(places(count) == 0, last, 0.0), axis=1, keepdims=True)
    return jnp.concatenate([pick, pick], axis=1), last


def turned(values):
    return jnp.concatenate(split(values.T), axis=1)


def quarters():
    for half in range(2):
        for t in range(2):
            yield slice(half * HB, half * HB + HB), slice(t * HB, t * HB + HB)


def skew(diag, ref):
    for rows, lanes in quarters():
        ref[rows, lanes] = pltpu.roll(diag[rows, lanes], 0, 1, stride=1, stride_axis=0)


def place_block(rolled, last, wh, wl, b):
    beyond = places(HB)
    parts = [rolled[rows, lanes].T for rows, lanes in quarters()]
    for half in range(2):
        rows = slice(half * HB, half * HB + HB)
        near, far = parts[2 * half : 2 * half + 2]
        edge = jnp.where(beyond == 0, last[:, rows], 0.0)
        tiles = [
            jnp.where(beyond <= 0, near, 0.0),
            jnp.where(beyond <= 0, far, near),
            jnp.where(beyond > 0, far, edge),
        ]
        for t, tile in enumerate(tiles):
            high, low = split(tile)
            for ref, part in ((wh, high), (wl, low)):
                ref[b, (half + t) * HB : (half + t + 1) * HB, rows] = part
        empty = 3 * HB * (1 - half)
        for ref in (wh, wl):
            ref[b, empty : empty + HB, rows] = jnp.zeros((HB, HB), jnp.bfloat16)


def final(values, last):
    return jnp.sum(values * last, axis=0, keepdims=True)


def blocks_kernel(band_ref, off_ref, wh, wl, both_ref, diag_ref, rolled_ref):
    pick, last = picker(off_ref)
    count = wh.shape[0]
    for b in range(count + 3):
        if b >= 3:
            values = band_ref[:, (b - 3) * WB : (b - 2) * WB]
            place_block(rolled_ref[(b - 3) % 2], final(values, last), wh, wl, b - 3)
        if 2 <= b < count + 2:
            skew(diag_ref[(b - 2) % 2], rolled_ref.at[(b - 2) % 2])
        if 1 <= b < count + 1:
            diag_ref[(b - 1) % 2] = mm(both_ref[(b - 1) % 2], pick, NT)
        if b < count:
            both_ref[b % 2] = turned(band_ref[:, b * WB : b * WB + WB])


def edges_kernel(src_ref, band_ref, up_ref, down_ref, sems):
    rows, width = src_ref.shape
    reach = 3 * HB
    copies = []
    for ref, far, near in ((up_ref, width - reach, width - WB), (down_ref, 0, 0)):
        parts = [(src_ref.at[:, pl.ds(far, reach)], ref.at[:, pl.ds(0, reach)])]
        for half in range(2):
            take = band_ref.at[pl.ds(half * rows, rows), pl.ds(near, WB)]
            parts.append((take, ref.at[:, pl.ds(reach + half * WB, WB)]))
        for one, two in parts:
            copies.append(pltpu.make_async_copy(one, two, sems.at[len(copies)]))
    for copy in copies:
        copy.start()
    for copy in copies:
        copy.wait()


def powers_kernel(
    total, src_ref, low_in, high_in, off_ref, wh, wl, high_ref, low_ref, gram_ref, xs, eh, el, rolled
):
    rows, width = src_ref.shape
    inner = width // WB
    reach = 3 * HB
    edges = [(low_in, 0, 0), (high_in, 1, reach + width)]
    for b in range(inner):
        at = slice(b * WB, b * WB + WB)
        into = slice(b * WB + reach, b * WB + reach + WB)
        high, low = split(src_ref[:, at])
        high_ref[:rows, at] = high
        low_ref[:rows, at] = low
        xs[0, :rows, into] = high
        xs[0, rows:, into] = low
    pick, last = picker(off_ref)
    sides = []
    for ref, side, at in edges:
        high, low = split(ref[:, :reach])
        xs[0, :rows, at : at + reach] = high
        xs[0, rows:, at : at + reach] = low
        values = jnp.concatenate([ref[:, reach : reach + WB], ref[:, reach + WB :]], axis=0)
        sides.append((values, mm(turned(values), pick, NT)))
    for side, (values, diag) in enumerate(sides):
        skew(diag, rolled.at[side])
    for side, (values, diag) in enumerate(sides):
        place_block(rolled[side], final(values, last), eh, el, side)
    for power in (1, 2):
        for at in (0, xs.shape[2] - HB):
            xs[power, :, at : at + HB] = jnp.zeros((2 * rows, HB), jnp.bfloat16)

    def apply(power, at, by_high, by_low):
        window = xs[power - 1, :, at : at + SPAN]
        both = mm(window, by_high)
        return split(both[:rows] + both[rows:] + mm(window[:rows], by_low))

    for power in (1, 2, 3):
        inside = list(range(2, inner)) + [1, inner]
        for b in inside + [0, inner + 1] * (power < 3):
            if b in (0, inner + 1):
                by = (eh[int(b > 0)], el[int(b > 0)])
            else:
                by = (wh[b - 1], wl[b - 1])
            pair = apply(power, b * WB, *by)
            if power < 3:
                for part in range(2):
                    place = slice(b * WB + HB, b * WB + HB + WB)
                    xs[power, part * rows : (part + 1) * rows, place] = pair[part]
            if 0 < b <= inner:
                for ref, value in zip((high_ref, low_ref), pair):
                    ref[power * rows : (power + 1) * rows, b * WB - WB : b * WB] = value
    tall = high_ref[...]
    gram = mm(tall, tall, NT) + 2.0 * mm(tall, low_ref[...], NT)
    pack(gram_ref, (gram + gram.T) * (0.5 / total))


def places(order):
    shape = (order, order)
    down = lax.broadcasted_iota(jnp.int32, shape, 0)
    return lax.broadcasted_iota(jnp.int32, shape, 1) - down


def pack(ref, gram):
    half = ref.shape[1]
    across = places(half)
    tail = gram[half:, half:]
    ref[:half] = gram[:half, half:]
    ref[half : 2 * half] = jnp.where(across >= 0, gram[:half, :half], tail)
    ref[2 * half :] = jnp.zeros((ref.shape[0] - 2 * half, half), jnp.float32)
    middle = jnp.sum(jnp.where(across == 0, tail, 0.0), axis=0, keepdims=True)
    ref[2 * half : 2 * half + 1] = middle


def unpack(ref):
    half = ref.shape[1]
    across = places(half)
    cross = ref[:half]
    both = ref[half : 2 * half]
    middle = jnp.broadcast_to(ref[2 * half : 2 * half + 1], (half, half))
    upper = jnp.where(across > 0, both, 0.0)
    lower = jnp.where(across < 0, both, 0.0)
    head = upper + upper.T + jnp.where(across == 0, both, 0.0)
    tail = lower + lower.T + jnp.where(across == 0, middle, 0.0)
    return head, cross, tail


def lane_copy(x, lane):
    return jnp.broadcast_to(x[:, lane : lane + 1], (8, 128))


def row_copy(x, row):
    return jnp.broadcast_to(x[row : row + 1, :], (8, 128))


def eliminate(work, tiles):
    order = work.shape[0]
    sub = lax.broadcasted_iota(jnp.int32, (8, 128), 0)

    def tile(g, t):
        return slice(8 * g, 8 * g + 8), slice(128 * t, 128 * t + 128)

    for kb in range(order // 8):
        own = [work[tile(kb, t)] for t in range(tiles)]
        cols = [lane_copy(own[0], 8 * kb + j) for j in range(8)]
        inverses, cross, tops = [], [], []
        pivots = jnp.ones((8, 128), jnp.float32)
        for k in range(8):
            pivot = row_copy(cols[k], k)
            inverse = 1.0 / pivot
            pivots = jnp.where(sub == k, pivot, pivots)
            m = jnp.where(sub > k, cols[k] * inverse, 0.0)
            crossing = [row_copy(cols[j], k) for j in range(k + 1, 8)]
            top = [row_copy(x, k) for x in own]
            for j in range(k + 1, 8):
                cols[j] = cols[j] - m * crossing[j - k - 1]
            own = [x - m * y for x, y in zip(own, top)]
            inverses.append(inverse)
            cross.append(crossing)
            tops.append(top)
        scale = lax.rsqrt(pivots)
        for t in range(1, tiles):
            work[tile(kb, t)] = own[t] * scale
        for g in range(kb + 1, order // 8):
            rest = [work[tile(g, t)] for t in range(tiles)]
            q = [lane_copy(rest[0], 8 * kb + j) for j in range(8)]
            for k in range(8):
                m = q[k] * inverses[k]
                for j in range(k + 1, 8):
                    q[j] = q[j] - m * cross[k][j - k - 1]
                rest = [x - m * y for x, y in zip(rest, tops[k])]
            for t in range(tiles):
                work[tile(g, t)] = rest[t]


def compress(gram, spanning, work):
    retain, order = spanning.shape
    metric = exact(exact(spanning, gram), spanning, NT)
    work[:, :retain] = 0.5 * (metric + metric.T)
    work[:, retain : retain + order] = spanning
    eliminate(work, (retain + order) // 128)
    return work[:, retain : retain + order]


def finish_kernel(gram_ref, high_ref, low_ref, out_ref, work, out, sems):
    keep = out_ref.shape[0]
    g11, g12, g22 = unpack(gram_ref)
    one = compress(g11, g11, work)
    one = compress(g11, exact(one, g11), work)
    cross = exact(exact(one, g12), one, NT)
    tail = exact(exact(one, g22), one, NT)
    same = jnp.where(places(keep) == 0, 1.0, 0.0)
    top = jnp.concatenate([same, cross], axis=1)
    bottom = jnp.concatenate([cross.T, tail], axis=1)
    gram = jnp.concatenate([top, bottom], axis=0)
    two = compress(gram, exact(top, gram), work)
    overall = jnp.concatenate([exact(two[:, :keep], one), exact(two[:, keep:], one)], axis=1)
    fh, fl = split(overall)
    both = jnp.concatenate([fh, fl], axis=0)

    quarter = out.shape[1] // 4
    stores = []
    for b in range(out.shape[1] // WB):
        place = slice(b * WB, b * WB + WB)
        wide = mm(both, high_ref[:, place])
        out[:, place] = wide[:keep] + wide[keep:] + mm(fh, low_ref[:, place])
        if (b + 1) * WB % quarter == 0:
            at = pl.ds((b + 1) * WB - quarter, quarter)
            sem = sems.at[len(stores)]
            stores.append(pltpu.make_async_copy(out.at[:, at], out_ref.at[:, at], sem))
            stores[-1].start()
    for store in stores:
        store.wait()


def sum_kernel(in_ref, out_ref):
    total = in_ref[0]
    for i in range(1, in_ref.shape[0]):
        total = total + in_ref[i]
    for i in range(out_ref.shape[0]):
        out_ref[i] = total


def exchange(blocks, axis):
    return lax.all_to_all(blocks, axis, 0, 0, tiled=True)


def summed_copies(blocks, axis):
    copies = pl.pallas_call(
        sum_kernel,
        out_shape=jax.ShapeDtypeStruct((lax.axis_size(axis), *blocks.shape[1:]), jnp.float32),
        compiler_params=pltpu.CompilerParams(vmem_limit_bytes=8 * 1024 * 1024),
        name="sums_" + axis,
    )(blocks)
    return exchange(copies, axis)


def body(source, band_values, offsets):
    devices = lax.axis_size(ROWS)
    group = lax.axis_size("near")
    rows, width = source.shape
    reach = 3 * HB
    inner = width // WB
    up = [(i, i + 1) for i in range(devices - 1)]
    down = [(i + 1, i) for i in range(devices - 1)]

    hbm = pl.BlockSpec(memory_space=pltpu.HBM)
    vmem = pl.BlockSpec(memory_space=pltpu.VMEM)
    edge = jax.ShapeDtypeStruct((rows, reach + 2 * WB), jnp.float32)
    last, first = pl.pallas_call(
        edges_kernel,
        out_shape=[edge, edge],
        in_specs=[hbm, hbm],
        scratch_shapes=[pltpu.SemaphoreType.DMA((6,))],
        compiler_params=pltpu.CompilerParams(vmem_limit_bytes=64_500_000),
        name="edges",
    )(source, band_values)
    low = lax.ppermute(last, ROWS, up)
    high = lax.ppermute(first, ROWS, down)
    offsets = offsets.reshape(1, -1)
    blocks = jax.ShapeDtypeStruct((inner, SPAN, WB), jnp.bfloat16)
    by_high, by_low = pl.pallas_call(
        blocks_kernel,
        out_shape=[blocks, blocks],
        scratch_shapes=[
            pltpu.VMEM((2, WB, 2 * HB), jnp.bfloat16),
            pltpu.VMEM((2, WB, 2 * HB), jnp.float32),
            pltpu.VMEM((2, WB, 2 * HB), jnp.float32),
        ],
        compiler_params=pltpu.CompilerParams(vmem_limit_bytes=12 * 1024 * 1024),
        cost_estimate=pl.CostEstimate(
            flops=10_000_000_000, bytes_accessed=12_000_000, transcendentals=0
        ),
        name="blocks",
    )(band_values, offsets)
    wide = width + 2 * reach
    high, low, gram = pl.pallas_call(
        functools.partial(powers_kernel, float(width * devices)),
        out_shape=[
            jax.ShapeDtypeStruct((4 * rows, width), jnp.bfloat16),
            jax.ShapeDtypeStruct((4 * rows, width), jnp.bfloat16),
            jax.ShapeDtypeStruct((4 * rows + 16, 2 * rows), jnp.float32),
        ],
        scratch_shapes=[
            pltpu.VMEM((3, 2 * rows, wide), jnp.bfloat16),
            pltpu.VMEM((2, SPAN, WB), jnp.bfloat16),
            pltpu.VMEM((2, SPAN, WB), jnp.bfloat16),
            pltpu.VMEM((2, WB, 2 * HB), jnp.float32),
        ],
        compiler_params=pltpu.CompilerParams(vmem_limit_bytes=16 * 1024 * 1024),
        name="powers",
    )(source, low, high, offsets, by_high, by_low)

    gram = exchange(gram.reshape(group, -1, 1, 2 * rows), "near")
    gram = summed_copies(summed_copies(gram, "far"), "near")
    gram = gram.reshape(4 * rows + 16, 2 * rows)

    return pl.pallas_call(
        finish_kernel,
        out_shape=jax.ShapeDtypeStruct((2 * rows, width), jnp.float32),
        out_specs=hbm,
        scratch_shapes=[
            pltpu.VMEM((2 * rows, 6 * rows), jnp.float32),
            pltpu.VMEM((2 * rows, width), jnp.float32),
            pltpu.SemaphoreType.DMA((4,)),
        ],
        compiler_params=pltpu.CompilerParams(vmem_limit_bytes=16 * 1024 * 1024),
        name="finish",
    )(gram, high, low)


def solution(mesh):
    devices = mesh.devices.size
    near = 1 << (devices.bit_length() // 2)
    grid = Mesh(mesh.devices.reshape(devices // near, near), ROWS)
    split_rows = P(None, ROWS)
    return jax.shard_map(
        body,
        mesh=grid,
        in_specs=(split_rows, split_rows, P()),
        out_specs=split_rows,
        check_vma=False,
    )
```

```python
import functools

import jax
import jax.numpy as jnp
from jax import lax
from jax.experimental import pallas as pl
from jax.experimental.pallas import tpu as pltpu
from jax.sharding import Mesh
from jax.sharding import PartitionSpec as P

HB = 128
WB = 256
SPAN = 2 * WB
ROWS = ("far", "near")
NN = (((1,), (0,)), ((), ()))
NT = (((1,), (1,)), ((), ()))


def split(x):
    high = x.astype(jnp.bfloat16)
    return high, (x - high.astype(jnp.float32)).astype(jnp.bfloat16)


def mm(a, b, dims=NN):
    return lax.dot_general(a, b, dims, preferred_element_type=jnp.float32)


def exact(a, b, dims=NN):
    return lax.dot_general(
        a, b, dims, precision=lax.Precision.HIGHEST, preferred_element_type=jnp.float32
    )


def picker(off_ref):
    count = off_ref.shape[1]
    down = lax.broadcasted_iota(jnp.int32, (2 * HB, count), 0)
    pick = jnp.where(down == off_ref[...] + HB, 1.0, 0.0).astype(jnp.bfloat16)
    last = jnp.where(off_ref[...] == HB, 1.0, 0.0)
    last = jnp.sum(jnp.where(places(count) == 0, last, 0.0), axis=1, keepdims=True)
    return jnp.concatenate([pick, pick], axis=1), last


def turned(values):
    return jnp.concatenate(split(values.T), axis=1)


def quarters():
    for half in range(2):
        for t in range(2):
            yield slice(half * HB, half * HB + HB), slice(t * HB, t * HB + HB)


def skew(diag, ref):
    for rows, lanes in quarters():
        ref[rows, lanes] = pltpu.roll(diag[rows, lanes], 0, 1, stride=1, stride_axis=0)


def place_block(rolled, last, wh, wl, b):
    beyond = places(HB)
    parts = [rolled[rows, lanes].T for rows, lanes in quarters()]
    for half in range(2):
        rows = slice(half * HB, half * HB + HB)
        near, far = parts[2 * half : 2 * half + 2]
        edge = jnp.where(beyond == 0, last[:, rows], 0.0)
        tiles = [
            jnp.where(beyond <= 0, near, 0.0),
            jnp.where(beyond <= 0, far, near),
            jnp.where(beyond > 0, far, edge),
        ]
        for t, tile in enumerate(tiles):
            high, low = split(tile)
            for ref, part in ((wh, high), (wl, low)):
                ref[b, (half + t) * HB : (half + t + 1) * HB, rows] = part
        empty = 3 * HB * (1 - half)
        for ref in (wh, wl):
            ref[b, empty : empty + HB, rows] = jnp.zeros((HB, HB), jnp.bfloat16)


def final(values, last):
    return jnp.sum(values * last, axis=0, keepdims=True)


def blocks_kernel(band_ref, off_ref, wh, wl, both_ref, diag_ref, rolled_ref):
    pick, last = picker(off_ref)
    count = wh.shape[0]
    for b in range(count + 3):
        if b >= 3:
            values = band_ref[:, (b - 3) * WB : (b - 2) * WB]
            place_block(rolled_ref[(b - 3) % 2], final(values, last), wh, wl, b - 3)
        if 2 <= b < count + 2:
            skew(diag_ref[(b - 2) % 2], rolled_ref.at[(b - 2) % 2])
        if 1 <= b < count + 1:
            diag_ref[(b - 1) % 2] = mm(both_ref[(b - 1) % 2], pick, NT)
        if b < count:
            both_ref[b % 2] = turned(band_ref[:, b * WB : b * WB + WB])


def edges_kernel(src_ref, band_ref, up_ref, down_ref, sems):
    rows, width = src_ref.shape
    reach = 3 * HB
    copies = []
    for ref, far, near in ((up_ref, width - reach, width - WB), (down_ref, 0, 0)):
        parts = [(src_ref.at[:, pl.ds(far, reach)], ref.at[:, pl.ds(0, reach)])]
        for half in range(2):
            take = band_ref.at[pl.ds(half * rows, rows), pl.ds(near, WB)]
            parts.append((take, ref.at[:, pl.ds(reach + half * WB, WB)]))
        for one, two in parts:
            copies.append(pltpu.make_async_copy(one, two, sems.at[len(copies)]))
    for copy in copies:
        copy.start()
    for copy in copies:
        copy.wait()


def powers_kernel(
    total, src_ref, low_in, high_in, off_ref, wh, wl, high_ref, low_ref, gram_ref, xs, eh, el, rolled
):
    rows, width = src_ref.shape
    inner = width // WB
    reach = 3 * HB
    edges = [(low_in, 0, 0), (high_in, 1, reach + width)]
    for b in range(inner):
        at = slice(b * WB, b * WB + WB)
        into = slice(b * WB + reach, b * WB + reach + WB)
        high, low = split(src_ref[:, at])
        high_ref[:rows, at] = high
        low_ref[:rows, at] = low
        xs[0, :rows, into] = high
        xs[0, rows:, into] = low
    pick, last = picker(off_ref)
    sides = []
    for ref, side, at in edges:
        high, low = split(ref[:, :reach])
        xs[0, :rows, at : at + reach] = high
        xs[0, rows:, at : at + reach] = low
        values = jnp.concatenate([ref[:, reach : reach + WB], ref[:, reach + WB :]], axis=0)
        sides.append((values, mm(turned(values), pick, NT)))
    for side, (values, diag) in enumerate(sides):
        skew(diag, rolled.at[side])
    for side, (values, diag) in enumerate(sides):
        place_block(rolled[side], final(values, last), eh, el, side)
    for power in (1, 2):
        for at in (0, xs.shape[2] - HB):
            xs[power, :, at : at + HB] = jnp.zeros((2 * rows, HB), jnp.bfloat16)

    def apply(power, at, by_high, by_low):
        window = xs[power - 1, :, at : at + SPAN]
        both = mm(window, by_high)
        return split(both[:rows] + both[rows:] + mm(window[:rows], by_low))

    for power in (1, 2, 3):
        inside = list(range(2, inner)) + [1, inner]
        for b in inside + [0, inner + 1] * (power < 3):
            if b in (0, inner + 1):
                by = (eh[int(b > 0)], el[int(b > 0)])
            else:
                by = (wh[b - 1], wl[b - 1])
            pair = apply(power, b * WB, *by)
            if power < 3:
                for part in range(2):
                    place = slice(b * WB + HB, b * WB + HB + WB)
                    xs[power, part * rows : (part + 1) * rows, place] = pair[part]
            if 0 < b <= inner:
                for ref, value in zip((high_ref, low_ref), pair):
                    ref[power * rows : (power + 1) * rows, b * WB - WB : b * WB] = value
    tall = high_ref[...]
    gram = mm(tall, tall, NT) + 2.0 * mm(tall, low_ref[...], NT)
    pack(gram_ref, (gram + gram.T) * (0.5 / total))


def places(order):
    shape = (order, order)
    down = lax.broadcasted_iota(jnp.int32, shape, 0)
    return lax.broadcasted_iota(jnp.int32, shape, 1) - down


def pack(ref, gram):
    half = ref.shape[1]
    across = places(half)
    tail = gram[half:, half:]
    ref[:half] = gram[:half, half:]
    ref[half : 2 * half] = jnp.where(across >= 0, gram[:half, :half], tail)
    ref[2 * half :] = jnp.zeros((ref.shape[0] - 2 * half, half), jnp.float32)
    middle = jnp.sum(jnp.where(across == 0, tail, 0.0), axis=0, keepdims=True)
    ref[2 * half : 2 * half + 1] = middle


def unpack(ref):
    half = ref.shape[1]
    across = places(half)
    cross = ref[:half]
    both = ref[half : 2 * half]
    middle = jnp.broadcast_to(ref[2 * half : 2 * half + 1], (half, half))
    upper = jnp.where(across > 0, both, 0.0)
    lower = jnp.where(across < 0, both, 0.0)
    head = upper + upper.T + jnp.where(across == 0, both, 0.0)
    tail = lower + lower.T + jnp.where(across == 0, middle, 0.0)
    return head, cross, tail


def lane_copy(x, lane):
    return jnp.broadcast_to(x[:, lane : lane + 1], (8, 128))


def row_copy(x, row):
    return jnp.broadcast_to(x[row : row + 1, :], (8, 128))


def eliminate(work, tiles):
    order = work.shape[0]
    sub = lax.broadcasted_iota(jnp.int32, (8, 128), 0)

    def tile(g, t):
        return slice(8 * g, 8 * g + 8), slice(128 * t, 128 * t + 128)

    for kb in range(order // 8):
        own = [work[tile(kb, t)] for t in range(tiles)]
        cols = [lane_copy(own[0], 8 * kb + j) for j in range(8)]
        inverses, cross, tops = [], [], []
        pivots = jnp.ones((8, 128), jnp.float32)
        for k in range(8):
            pivot = row_copy(cols[k], k)
            inverse = 1.0 / pivot
            pivots = jnp.where(sub == k, pivot, pivots)
            m = jnp.where(sub > k, cols[k] * inverse, 0.0)
            crossing = [row_copy(cols[j], k) for j in range(k + 1, 8)]
            top = [row_copy(x, k) for x in own]
            for j in range(k + 1, 8):
                cols[j] = cols[j] - m * crossing[j - k - 1]
            own = [x - m * y for x, y in zip(own, top)]
            inverses.append(inverse)
            cross.append(crossing)
            tops.append(top)
        scale = lax.rsqrt(pivots)
        for t in range(1, tiles):
            work[tile(kb, t)] = own[t] * scale
        for g in range(kb + 1, order // 8):
            rest = [work[tile(g, t)] for t in range(tiles)]
            q = [lane_copy(rest[0], 8 * kb + j) for j in range(8)]
            for k in range(8):
                m = q[k] * inverses[k]
                for j in range(k + 1, 8):
                    q[j] = q[j] - m * cross[k][j - k - 1]
                rest = [x - m * y for x, y in zip(rest, tops[k])]
            for t in range(tiles):
                work[tile(g, t)] = rest[t]


def solve(metric, image, work):
    order, width = image.shape
    work[:, :order] = metric
    work[:, order : order + width] = image
    eliminate(work, (order + width) // 128)
    return work[:, order : order + width]


def finish_kernel(gram_ref, high_ref, low_ref, out_ref, work, out, sems):
    keep = out_ref.shape[0]
    g11, g12, g22 = unpack(gram_ref)
    square = exact(g11, g11)
    span = solve(exact(square, g11, NT), square, work)
    one = solve(exact(exact(span, g11), span, NT), span, work)
    cross = exact(exact(one, g12), one, NT)
    tail = exact(exact(one, g22), one, NT)
    same = jnp.where(places(keep) == 0, 1.0, 0.0)
    top = jnp.concatenate([same, cross], axis=1)
    bottom = jnp.concatenate([cross.T, tail], axis=1)
    gram = jnp.concatenate([top, bottom], axis=0)
    span = exact(top, gram)
    image = jnp.concatenate([exact(span[:, :keep], one), exact(span[:, keep:], one)], axis=1)
    overall = solve(exact(exact(span, gram), span, NT), image, work)
    fh, fl = split(overall)
    both = jnp.concatenate([fh, fl], axis=0)

    quarter = out.shape[1] // 4
    stores = []
    for b in range(out.shape[1] // WB):
        place = slice(b * WB, b * WB + WB)
        wide = mm(both, high_ref[:, place])
        out[:, place] = wide[:keep] + wide[keep:] + mm(fh, low_ref[:, place])
        if (b + 1) * WB % quarter == 0:
            at = pl.ds((b + 1) * WB - quarter, quarter)
            sem = sems.at[len(stores)]
            stores.append(pltpu.make_async_copy(out.at[:, at], out_ref.at[:, at], sem))
            stores[-1].start()
    for store in stores:
        store.wait()


def sum_kernel(in_ref, out_ref):
    total = in_ref[0]
    for i in range(1, in_ref.shape[0]):
        total = total + in_ref[i]
    for i in range(out_ref.shape[0]):
        out_ref[i] = total


def exchange(blocks, axis):
    return lax.all_to_all(blocks, axis, 0, 0, tiled=True)


def summed_copies(blocks, axis):
    copies = pl.pallas_call(
        sum_kernel,
        out_shape=jax.ShapeDtypeStruct((lax.axis_size(axis), *blocks.shape[1:]), jnp.float32),
        compiler_params=pltpu.CompilerParams(vmem_limit_bytes=8 * 1024 * 1024),
        name="sums_" + axis,
    )(blocks)
    return exchange(copies, axis)


def body(source, band_values, offsets):
    devices = lax.axis_size(ROWS)
    group = lax.axis_size("far")
    rows, width = source.shape
    reach = 3 * HB
    inner = width // WB
    up = [(i, i + 1) for i in range(devices - 1)]
    down = [(i + 1, i) for i in range(devices - 1)]

    hbm = pl.BlockSpec(memory_space=pltpu.HBM)
    vmem = pl.BlockSpec(memory_space=pltpu.VMEM)
    edge = jax.ShapeDtypeStruct((rows, reach + 2 * WB), jnp.float32)
    last, first = pl.pallas_call(
        edges_kernel,
        out_shape=[edge, edge],
        in_specs=[hbm, hbm],
        scratch_shapes=[pltpu.SemaphoreType.DMA((6,))],
        compiler_params=pltpu.CompilerParams(vmem_limit_bytes=64_500_000),
        name="edges",
    )(source, band_values)
    low = lax.ppermute(last, ROWS, up)
    high = lax.ppermute(first, ROWS, down)
    offsets = offsets.reshape(1, -1)
    blocks = jax.ShapeDtypeStruct((inner, SPAN, WB), jnp.bfloat16)
    by_high, by_low = pl.pallas_call(
        blocks_kernel,
        out_shape=[blocks, blocks],
        scratch_shapes=[
            pltpu.VMEM((2, WB, 2 * HB), jnp.bfloat16),
            pltpu.VMEM((2, WB, 2 * HB), jnp.float32),
            pltpu.VMEM((2, WB, 2 * HB), jnp.float32),
        ],
        compiler_params=pltpu.CompilerParams(vmem_limit_bytes=12 * 1024 * 1024),
        cost_estimate=pl.CostEstimate(
            flops=10_000_000_000, bytes_accessed=12_000_000, transcendentals=0
        ),
        name="blocks",
    )(band_values, offsets)
    wide = width + 2 * reach
    high, low, gram = pl.pallas_call(
        functools.partial(powers_kernel, float(width * devices)),
        out_shape=[
            jax.ShapeDtypeStruct((4 * rows, width), jnp.bfloat16),
            jax.ShapeDtypeStruct((4 * rows, width), jnp.bfloat16),
            jax.ShapeDtypeStruct((4 * rows + 16, 2 * rows), jnp.float32),
        ],
        scratch_shapes=[
            pltpu.VMEM((3, 2 * rows, wide), jnp.bfloat16),
            pltpu.VMEM((2, SPAN, WB), jnp.bfloat16),
            pltpu.VMEM((2, SPAN, WB), jnp.bfloat16),
            pltpu.VMEM((2, WB, 2 * HB), jnp.float32),
        ],
        compiler_params=pltpu.CompilerParams(vmem_limit_bytes=16 * 1024 * 1024),
        name="powers",
    )(source, low, high, offsets, by_high, by_low)

    gram = exchange(gram.reshape(group, -1, 1, 2 * rows), "far")
    gram = summed_copies(summed_copies(gram, "near"), "far")
    gram = gram.reshape(4 * rows + 16, 2 * rows)

    return pl.pallas_call(
        finish_kernel,
        out_shape=jax.ShapeDtypeStruct((2 * rows, width), jnp.float32),
        out_specs=hbm,
        scratch_shapes=[
            pltpu.VMEM((2 * rows, 6 * rows), jnp.float32),
            pltpu.VMEM((2 * rows, width), jnp.float32),
            pltpu.SemaphoreType.DMA((4,)),
        ],
        compiler_params=pltpu.CompilerParams(vmem_limit_bytes=16 * 1024 * 1024),
        name="finish",
    )(gram, high, low)


def solution(mesh):
    devices = mesh.devices.size
    near = 1 << (devices.bit_length() // 2)
    grid = Mesh(mesh.devices.reshape(devices // near, near), ROWS)
    split_rows = P(None, ROWS)
    return jax.shard_map(
        body,
        mesh=grid,
        in_specs=(split_rows, split_rows, P()),
        out_specs=split_rows,
        check_vma=False,
    )
```

```python
import functools

import jax
import jax.numpy as jnp
from jax import lax
from jax.experimental import pallas as pl
from jax.experimental.pallas import tpu as pltpu
from jax.sharding import Mesh
from jax.sharding import PartitionSpec as P

HB = 128
WB = 256
SPAN = 2 * WB
ROWS = ("far", "near")
NN = (((1,), (0,)), ((), ()))
NT = (((1,), (1,)), ((), ()))


def split(x):
    high = x.astype(jnp.bfloat16)
    return high, (x - high.astype(jnp.float32)).astype(jnp.bfloat16)


def mm(a, b, dims=NN):
    return lax.dot_general(a, b, dims, preferred_element_type=jnp.float32)


def exact(a, b, dims=NN):
    return lax.dot_general(
        a, b, dims, precision=lax.Precision.HIGHEST, preferred_element_type=jnp.float32
    )


def picker(off_ref):
    count = off_ref.shape[1]
    down = lax.broadcasted_iota(jnp.int32, (2 * HB, count), 0)
    pick = jnp.where(down == off_ref[...] + HB, 1.0, 0.0).astype(jnp.bfloat16)
    last = jnp.where(off_ref[...] == HB, 1.0, 0.0)
    last = jnp.sum(jnp.where(places(count) == 0, last, 0.0), axis=1, keepdims=True)
    return jnp.concatenate([pick, pick], axis=1), last


def turned(values):
    return jnp.concatenate(split(values.T), axis=1)


def quarters():
    for half in range(2):
        for t in range(2):
            yield slice(half * HB, half * HB + HB), slice(t * HB, t * HB + HB)


def skew(diag, ref):
    for rows, lanes in quarters():
        ref[rows, lanes] = pltpu.roll(diag[rows, lanes], 0, 1, stride=1, stride_axis=0)


def place_block(rolled, last, wh, wl, b):
    beyond = places(HB)
    parts = [rolled[rows, lanes].T for rows, lanes in quarters()]
    for half in range(2):
        rows = slice(half * HB, half * HB + HB)
        near, far = parts[2 * half : 2 * half + 2]
        edge = jnp.where(beyond == 0, last[:, rows], 0.0)
        tiles = [
            jnp.where(beyond <= 0, near, 0.0),
            jnp.where(beyond <= 0, far, near),
            jnp.where(beyond > 0, far, edge),
        ]
        for t, tile in enumerate(tiles):
            high, low = split(tile)
            for ref, part in ((wh, high), (wl, low)):
                ref[b, (half + t) * HB : (half + t + 1) * HB, rows] = part
        empty = 3 * HB * (1 - half)
        for ref in (wh, wl):
            ref[b, empty : empty + HB, rows] = jnp.zeros((HB, HB), jnp.bfloat16)


def final(values, last):
    return jnp.sum(values * last, axis=0, keepdims=True)


def blocks_kernel(band_ref, off_ref, wh, wl, both_ref, diag_ref, rolled_ref):
    pick, last = picker(off_ref)
    count = wh.shape[0]
    for b in range(count + 3):
        if b >= 3:
            values = band_ref[:, (b - 3) * WB : (b - 2) * WB]
            place_block(rolled_ref[(b - 3) % 2], final(values, last), wh, wl, b - 3)
        if 2 <= b < count + 2:
            skew(diag_ref[(b - 2) % 2], rolled_ref.at[(b - 2) % 2])
        if 1 <= b < count + 1:
            diag_ref[(b - 1) % 2] = mm(both_ref[(b - 1) % 2], pick, NT)
        if b < count:
            both_ref[b % 2] = turned(band_ref[:, b * WB : b * WB + WB])


def edges_kernel(src_ref, band_ref, up_ref, down_ref, sems):
    rows, width = src_ref.shape
    reach = 3 * HB
    copies = []
    for ref, far, near in ((up_ref, width - reach, width - WB), (down_ref, 0, 0)):
        parts = [(src_ref.at[:, pl.ds(far, reach)], ref.at[:, pl.ds(0, reach)])]
        for half in range(2):
            take = band_ref.at[pl.ds(half * rows, rows), pl.ds(near, WB)]
            parts.append((take, ref.at[:, pl.ds(reach + half * WB, WB)]))
        for one, two in parts:
            copies.append(pltpu.make_async_copy(one, two, sems.at[len(copies)]))
    for copy in copies:
        copy.start()
    for copy in copies:
        copy.wait()


def powers_kernel(
    total, src_ref, low_in, high_in, off_ref, wh, wl, high_ref, low_ref, gram_ref, xs, eh, el, rolled
):
    rows, width = src_ref.shape
    inner = width // WB
    reach = 3 * HB
    edges = [(low_in, 0, 0), (high_in, 1, reach + width)]
    for b in range(inner):
        at = slice(b * WB, b * WB + WB)
        into = slice(b * WB + reach, b * WB + reach + WB)
        high, low = split(src_ref[:, at])
        high_ref[:rows, at] = high
        low_ref[:rows, at] = low
        xs[0, :rows, into] = high
        xs[0, rows:, into] = low
    pick, last = picker(off_ref)
    sides = []
    for ref, side, at in edges:
        high, low = split(ref[:, :reach])
        xs[0, :rows, at : at + reach] = high
        xs[0, rows:, at : at + reach] = low
        values = jnp.concatenate([ref[:, reach : reach + WB], ref[:, reach + WB :]], axis=0)
        sides.append((values, mm(turned(values), pick, NT)))
    for side, (values, diag) in enumerate(sides):
        skew(diag, rolled.at[side])
    for side, (values, diag) in enumerate(sides):
        place_block(rolled[side], final(values, last), eh, el, side)
    for power in (1, 2):
        for at in (0, xs.shape[2] - HB):
            xs[power, :, at : at + HB] = jnp.zeros((2 * rows, HB), jnp.bfloat16)

    def apply(power, at, by_high, by_low):
        window = xs[power - 1, :, at : at + SPAN]
        both = mm(window, by_high)
        return split(both[:rows] + both[rows:] + mm(window[:rows], by_low))

    for power in (1, 2, 3):
        inside = list(range(2, inner)) + [1, inner]
        for b in inside + [0, inner + 1] * (power < 3):
            if b in (0, inner + 1):
                by = (eh[int(b > 0)], el[int(b > 0)])
            else:
                by = (wh[b - 1], wl[b - 1])
            pair = apply(power, b * WB, *by)
            if power < 3:
                for part in range(2):
                    place = slice(b * WB + HB, b * WB + HB + WB)
                    xs[power, part * rows : (part + 1) * rows, place] = pair[part]
            if 0 < b <= inner:
                for ref, value in zip((high_ref, low_ref), pair):
                    ref[power * rows : (power + 1) * rows, b * WB - WB : b * WB] = value
    tall = high_ref[...]
    gram = mm(tall, tall, NT) + 2.0 * mm(tall, low_ref[...], NT)
    pack(gram_ref, (gram + gram.T) * (0.5 / total))


def places(order):
    shape = (order, order)
    down = lax.broadcasted_iota(jnp.int32, shape, 0)
    return lax.broadcasted_iota(jnp.int32, shape, 1) - down


def pack(ref, gram):
    half = ref.shape[1]
    across = places(half)
    tail = gram[half:, half:]
    ref[:half] = gram[:half, half:]
    ref[half : 2 * half] = jnp.where(across >= 0, gram[:half, :half], tail)
    ref[2 * half :] = jnp.zeros((ref.shape[0] - 2 * half, half), jnp.float32)
    middle = jnp.sum(jnp.where(across == 0, tail, 0.0), axis=0, keepdims=True)
    ref[2 * half : 2 * half + 1] = middle


def unpack(ref):
    half = ref.shape[1]
    across = places(half)
    cross = ref[:half]
    both = ref[half : 2 * half]
    middle = jnp.broadcast_to(ref[2 * half : 2 * half + 1], (half, half))
    upper = jnp.where(across > 0, both, 0.0)
    lower = jnp.where(across < 0, both, 0.0)
    head = upper + upper.T + jnp.where(across == 0, both, 0.0)
    tail = lower + lower.T + jnp.where(across == 0, middle, 0.0)
    return head, cross, tail


def lane_copy(x, lane):
    return jnp.broadcast_to(x[:, lane : lane + 1], (8, 128))


def row_copy(x, row):
    return jnp.broadcast_to(x[row : row + 1, :], (8, 128))


def eliminate(work, tiles):
    order = work.shape[0]
    sub = lax.broadcasted_iota(jnp.int32, (8, 128), 0)

    def tile(g, t):
        return slice(8 * g, 8 * g + 8), slice(128 * t, 128 * t + 128)

    for kb in range(order // 8):
        own = [work[tile(kb, t)] for t in range(tiles)]
        cols = [lane_copy(own[0], 8 * kb + j) for j in range(8)]
        inverses, cross, tops = [], [], []
        pivots = jnp.ones((8, 128), jnp.float32)
        for k in range(8):
            pivot = row_copy(cols[k], k)
            inverse = 1.0 / pivot
            pivots = jnp.where(sub == k, pivot, pivots)
            m = jnp.where(sub > k, cols[k] * inverse, 0.0)
            crossing = [row_copy(cols[j], k) for j in range(k + 1, 8)]
            top = [row_copy(x, k) for x in own]
            for j in range(k + 1, 8):
                cols[j] = cols[j] - m * crossing[j - k - 1]
            own = [x - m * y for x, y in zip(own, top)]
            inverses.append(inverse)
            cross.append(crossing)
            tops.append(top)
        scale = lax.rsqrt(pivots)
        for t in range(1, tiles):
            work[tile(kb, t)] = own[t] * scale
        for g in range(kb + 1, order // 8):
            rest = [work[tile(g, t)] for t in range(tiles)]
            q = [lane_copy(rest[0], 8 * kb + j) for j in range(8)]
            for k in range(8):
                m = q[k] * inverses[k]
                for j in range(k + 1, 8):
                    q[j] = q[j] - m * cross[k][j - k - 1]
                rest = [x - m * y for x, y in zip(rest, tops[k])]
            for t in range(tiles):
                work[tile(g, t)] = rest[t]


def solve(metric, image, work):
    order, width = image.shape
    work[:, :order] = metric
    work[:, order : order + width] = image
    eliminate(work, (order + width) // 128)
    return work[:, order : order + width]


def finish_kernel(gram_ref, high_ref, low_ref, out_ref, work, out, sems):
    keep = out_ref.shape[0]
    g11, g12, g22 = unpack(gram_ref)
    square = exact(g11, g11)
    span = solve(exact(square, g11, NT), square, work)
    one = solve(exact(exact(span, g11), span, NT), span, work)
    cross = exact(exact(one, g12), one, NT)
    tail = exact(exact(one, g22), one, NT)
    same = jnp.where(places(keep) == 0, 1.0, 0.0)
    top = jnp.concatenate([same, cross], axis=1)
    bottom = jnp.concatenate([cross.T, tail], axis=1)
    gram = jnp.concatenate([top, bottom], axis=0)
    span = exact(top, gram)
    image = jnp.concatenate([exact(span[:, :keep], one), exact(span[:, keep:], one)], axis=1)
    overall = solve(exact(exact(span, gram), span, NT), image, work)
    fh, fl = split(overall)
    both = jnp.concatenate([fh, fl], axis=0)

    quarter = out.shape[1] // 4
    stores = []
    for b in range(out.shape[1] // WB):
        place = slice(b * WB, b * WB + WB)
        wide = mm(both, high_ref[:, place])
        out[:, place] = wide[:keep] + wide[keep:] + mm(fh, low_ref[:, place])
        if (b + 1) * WB % quarter == 0:
            at = pl.ds((b + 1) * WB - quarter, quarter)
            sem = sems.at[len(stores)]
            stores.append(pltpu.make_async_copy(out.at[:, at], out_ref.at[:, at], sem))
            stores[-1].start()
    for store in stores:
        store.wait()


def sum_kernel(in_ref, out_ref):
    total = in_ref[0]
    for i in range(1, in_ref.shape[0]):
        total = total + in_ref[i]
    for i in range(out_ref.shape[0]):
        out_ref[i] = total


def exchange(blocks, axis):
    return lax.all_to_all(blocks, axis, 0, 0, tiled=True)


def summed_copies(blocks, axis):
    copies = pl.pallas_call(
        sum_kernel,
        out_shape=jax.ShapeDtypeStruct((lax.axis_size(axis), *blocks.shape[1:]), jnp.float32),
        compiler_params=pltpu.CompilerParams(vmem_limit_bytes=8 * 1024 * 1024),
        name="sums_" + axis,
    )(blocks)
    return exchange(copies, axis)


def body(source, band_values, offsets):
    devices = lax.axis_size(ROWS)
    group = lax.axis_size("far")
    rows, width = source.shape
    reach = 3 * HB
    inner = width // WB
    up = [(i, i + 1) for i in range(devices - 1)]
    down = [(i + 1, i) for i in range(devices - 1)]

    hbm = pl.BlockSpec(memory_space=pltpu.HBM)
    vmem = pl.BlockSpec(memory_space=pltpu.VMEM)
    edge = jax.ShapeDtypeStruct((rows, reach + 2 * WB), jnp.float32)
    last, first = pl.pallas_call(
        edges_kernel,
        out_shape=[edge, edge],
        in_specs=[hbm, hbm],
        scratch_shapes=[pltpu.SemaphoreType.DMA((6,))],
        compiler_params=pltpu.CompilerParams(vmem_limit_bytes=4 * 1024 * 1024),
        name="edges",
    )(*[pltpu.with_memory_space_constraint(x, pltpu.HBM) for x in (source, band_values)])
    low = lax.ppermute(last, ROWS, up)
    high = lax.ppermute(first, ROWS, down)
    offsets = offsets.reshape(1, -1)
    blocks = jax.ShapeDtypeStruct((inner, SPAN, WB), jnp.bfloat16)
    by_high, by_low = pl.pallas_call(
        blocks_kernel,
        out_shape=[blocks, blocks],
        scratch_shapes=[
            pltpu.VMEM((2, WB, 2 * HB), jnp.bfloat16),
            pltpu.VMEM((2, WB, 2 * HB), jnp.float32),
            pltpu.VMEM((2, WB, 2 * HB), jnp.float32),
        ],
        compiler_params=pltpu.CompilerParams(vmem_limit_bytes=12 * 1024 * 1024),
        cost_estimate=pl.CostEstimate(
            flops=10_000_000_000, bytes_accessed=12_000_000, transcendentals=0
        ),
        name="blocks",
    )(band_values, offsets)
    wide = width + 2 * reach
    high, low, gram = pl.pallas_call(
        functools.partial(powers_kernel, float(width * devices)),
        out_shape=[
            jax.ShapeDtypeStruct((4 * rows, width), jnp.bfloat16),
            jax.ShapeDtypeStruct((4 * rows, width), jnp.bfloat16),
            jax.ShapeDtypeStruct((4 * rows + 16, 2 * rows), jnp.float32),
        ],
        scratch_shapes=[
            pltpu.VMEM((3, 2 * rows, wide), jnp.bfloat16),
            pltpu.VMEM((2, SPAN, WB), jnp.bfloat16),
            pltpu.VMEM((2, SPAN, WB), jnp.bfloat16),
            pltpu.VMEM((2, WB, 2 * HB), jnp.float32),
        ],
        compiler_params=pltpu.CompilerParams(vmem_limit_bytes=16 * 1024 * 1024),
        name="powers",
    )(source, low, high, offsets, by_high, by_low)

    gram = exchange(gram.reshape(group, -1, 1, 2 * rows), "far")
    gram = summed_copies(summed_copies(gram, "near"), "far")
    gram = gram.reshape(4 * rows + 16, 2 * rows)

    return pl.pallas_call(
        finish_kernel,
        out_shape=jax.ShapeDtypeStruct((2 * rows, width), jnp.float32),
        out_specs=hbm,
        scratch_shapes=[
            pltpu.VMEM((2 * rows, 6 * rows), jnp.float32),
            pltpu.VMEM((2 * rows, width), jnp.float32),
            pltpu.SemaphoreType.DMA((4,)),
        ],
        compiler_params=pltpu.CompilerParams(vmem_limit_bytes=16 * 1024 * 1024),
        name="finish",
    )(gram, high, low)


def solution(mesh):
    devices = mesh.devices.size
    near = 1 << (devices.bit_length() // 2)
    grid = Mesh(mesh.devices.reshape(devices // near, near), ROWS)
    split_rows = P(None, ROWS)
    return jax.shard_map(
        body,
        mesh=grid,
        in_specs=(split_rows, split_rows, P()),
        out_specs=split_rows,
        check_vma=False,
    )
```

```python
import functools

import jax
import jax.numpy as jnp
from jax import lax
from jax.experimental import pallas as pl
from jax.experimental.pallas import tpu as pltpu
from jax.sharding import Mesh
from jax.sharding import PartitionSpec as P

HB = 128
WB = 256
SPAN = 2 * WB
ROWS = ("far", "near")
NN = (((1,), (0,)), ((), ()))
NT = (((1,), (1,)), ((), ()))


def split(x):
    high = x.astype(jnp.bfloat16)
    return high, (x - high.astype(jnp.float32)).astype(jnp.bfloat16)


def mm(a, b, dims=NN):
    return lax.dot_general(a, b, dims, preferred_element_type=jnp.float32)


def exact(a, b, dims=NN):
    return lax.dot_general(
        a, b, dims, precision=lax.Precision.HIGHEST, preferred_element_type=jnp.float32
    )


def picker(off_ref):
    count = off_ref.shape[1]
    down = lax.broadcasted_iota(jnp.int32, (2 * HB, count), 0)
    pick = jnp.where(down == off_ref[...] + HB, 1.0, 0.0).astype(jnp.bfloat16)
    last = jnp.where(off_ref[...] == HB, 1.0, 0.0)
    last = jnp.sum(jnp.where(places(count) == 0, last, 0.0), axis=1, keepdims=True)
    return jnp.concatenate([pick, pick], axis=1), last


def turned(values):
    return jnp.concatenate(split(values.T), axis=1)


def quarters():
    for half in range(2):
        for t in range(2):
            yield slice(half * HB, half * HB + HB), slice(t * HB, t * HB + HB)


def skew(diag, ref):
    for rows, lanes in quarters():
        ref[rows, lanes] = pltpu.roll(diag[rows, lanes], 0, 1, stride=1, stride_axis=0)


def place_block(rolled, last, wh, wl, b):
    beyond = places(HB)
    parts = [rolled[rows, lanes].T for rows, lanes in quarters()]
    for half in range(2):
        rows = slice(half * HB, half * HB + HB)
        near, far = parts[2 * half : 2 * half + 2]
        edge = jnp.where(beyond == 0, last[:, rows], 0.0)
        tiles = [
            jnp.where(beyond <= 0, near, 0.0),
            jnp.where(beyond <= 0, far, near),
            jnp.where(beyond > 0, far, edge),
        ]
        for t, tile in enumerate(tiles):
            high, low = split(tile)
            for ref, part in ((wh, high), (wl, low)):
                ref[b, (half + t) * HB : (half + t + 1) * HB, rows] = part
        empty = 3 * HB * (1 - half)
        for ref in (wh, wl):
            ref[b, empty : empty + HB, rows] = jnp.zeros((HB, HB), jnp.bfloat16)


def final(values, last):
    return jnp.sum(values * last, axis=0, keepdims=True)


def blocks_kernel(
    band_ref, off_ref, src_ref, wh, wl, s_ref, a_ref, both_ref, diag_ref, rolled_ref
):
    pick, last = picker(off_ref)
    count = wh.shape[0]
    rows = src_ref.shape[0]
    for b in range(count + 3):
        if 5 <= b:
            k = b - 4
            pair = applied(s_ref[:, k * WB - HB : k * WB - HB + SPAN], wh[k], wl[k])
            for part in range(2):
                a_ref[part * rows : (part + 1) * rows, k * WB : k * WB + WB] = pair[part]
        if 3 <= b:
            values = band_ref[:, (b - 3) * WB : (b - 2) * WB]
            place_block(rolled_ref[(b - 3) % 2], final(values, last), wh, wl, b - 3)
        if 2 <= b < count + 2:
            skew(diag_ref[(b - 2) % 2], rolled_ref.at[(b - 2) % 2])
        if 1 <= b < count + 1:
            diag_ref[(b - 1) % 2] = mm(both_ref[(b - 1) % 2], pick, NT)
        if b < count:
            at = slice(b * WB, b * WB + WB)
            both_ref[b % 2] = turned(band_ref[:, at])
            s_ref[:rows, at], s_ref[rows:, at] = split(src_ref[:, at])


def applied(window, by_high, by_low):
    rows = window.shape[0] // 2
    both = mm(window, by_high)
    return split(both[:rows] + both[rows:] + mm(window[:rows], by_low))


def edges_kernel(src_ref, band_ref, up_ref, down_ref, sems):
    rows, width = src_ref.shape
    reach = 3 * HB
    copies = []
    for ref, far, near in ((up_ref, width - reach, width - WB), (down_ref, 0, 0)):
        parts = [(src_ref.at[:, pl.ds(far, reach)], ref.at[:, pl.ds(0, reach)])]
        for half in range(2):
            take = band_ref.at[pl.ds(half * rows, rows), pl.ds(near, WB)]
            parts.append((take, ref.at[:, pl.ds(reach + half * WB, WB)]))
        for one, two in parts:
            copies.append(pltpu.make_async_copy(one, two, sems.at[len(copies)]))
    for copy in copies:
        copy.start()
    for copy in copies:
        copy.wait()


def powers_kernel(
    total, s_ref, a_ref, low_in, high_in, off_ref, wh, wl, high_ref, low_ref, gram_ref, xs, eh, el, rolled
):
    rows, width = s_ref.shape[0] // 2, s_ref.shape[1]
    inner = width // WB
    reach = 3 * HB
    edges = [(low_in, 0, 0), (high_in, 1, reach + width)]
    for b in range(inner):
        at = slice(b * WB, b * WB + WB)
        into = slice(b * WB + reach, b * WB + reach + WB)
        high_ref[:rows, at] = s_ref[:rows, at]
        low_ref[:rows, at] = s_ref[rows:, at]
        xs[0, :, into] = s_ref[:, at]
    pick, last = picker(off_ref)
    sides = []
    for ref, side, at in edges:
        high, low = split(ref[:, :reach])
        xs[0, :rows, at : at + reach] = high
        xs[0, rows:, at : at + reach] = low
        values = jnp.concatenate([ref[:, reach : reach + WB], ref[:, reach + WB :]], axis=0)
        sides.append((values, mm(turned(values), pick, NT)))
    for side, (values, diag) in enumerate(sides):
        skew(diag, rolled.at[side])
    for side, (values, diag) in enumerate(sides):
        place_block(rolled[side], final(values, last), eh, el, side)
    for power in (1, 2):
        for at in (0, xs.shape[2] - HB):
            xs[power, :, at : at + HB] = jnp.zeros((2 * rows, HB), jnp.bfloat16)

    for power in (1, 2, 3):
        inside = list(range(2, inner)) + [1, inner]
        for b in inside + [0, inner + 1] * (power < 3):
            if b in (0, inner + 1):
                by = (eh[int(b > 0)], el[int(b > 0)])
            else:
                by = (wh[b - 1], wl[b - 1])
            if power == 1 and 1 < b < inner:
                at = slice(b * WB - WB, b * WB)
                pair = a_ref[:rows, at], a_ref[rows:, at]
            else:
                pair = applied(xs[power - 1, :, b * WB : b * WB + SPAN], *by)
            if power < 3:
                for part in range(2):
                    place = slice(b * WB + HB, b * WB + HB + WB)
                    xs[power, part * rows : (part + 1) * rows, place] = pair[part]
            if 0 < b <= inner:
                for ref, value in zip((high_ref, low_ref), pair):
                    ref[power * rows : (power + 1) * rows, b * WB - WB : b * WB] = value
    tall = high_ref[...]
    gram = mm(tall, tall, NT) + 2.0 * mm(tall, low_ref[...], NT)
    pack(gram_ref, (gram + gram.T) * (0.5 / total))


def places(order):
    shape = (order, order)
    down = lax.broadcasted_iota(jnp.int32, shape, 0)
    return lax.broadcasted_iota(jnp.int32, shape, 1) - down


def pack(ref, gram):
    half = ref.shape[1]
    across = places(half)
    tail = gram[half:, half:]
    ref[:half] = gram[:half, half:]
    ref[half : 2 * half] = jnp.where(across >= 0, gram[:half, :half], tail)
    ref[2 * half :] = jnp.zeros((ref.shape[0] - 2 * half, half), jnp.float32)
    middle = jnp.sum(jnp.where(across == 0, tail, 0.0), axis=0, keepdims=True)
    ref[2 * half : 2 * half + 1] = middle


def unpack(ref):
    half = ref.shape[1]
    across = places(half)
    cross = ref[:half]
    both = ref[half : 2 * half]
    middle = jnp.broadcast_to(ref[2 * half : 2 * half + 1], (half, half))
    upper = jnp.where(across > 0, both, 0.0)
    lower = jnp.where(across < 0, both, 0.0)
    head = upper + upper.T + jnp.where(across == 0, both, 0.0)
    tail = lower + lower.T + jnp.where(across == 0, middle, 0.0)
    return head, cross, tail


def lane_copy(x, lane):
    return jnp.broadcast_to(x[:, lane : lane + 1], (8, 128))


def row_copy(x, row):
    return jnp.broadcast_to(x[row : row + 1, :], (8, 128))


def eliminate(work, tiles):
    order = work.shape[0]
    sub = lax.broadcasted_iota(jnp.int32, (8, 128), 0)

    def tile(g, t):
        return slice(8 * g, 8 * g + 8), slice(128 * t, 128 * t + 128)

    for kb in range(order // 8):
        own = [work[tile(kb, t)] for t in range(tiles)]
        cols = [lane_copy(own[0], 8 * kb + j) for j in range(8)]
        inverses, cross, tops = [], [], []
        pivots = jnp.ones((8, 128), jnp.float32)
        for k in range(8):
            pivot = row_copy(cols[k], k)
            inverse = 1.0 / pivot
            pivots = jnp.where(sub == k, pivot, pivots)
            m = jnp.where(sub > k, cols[k] * inverse, 0.0)
            crossing = [row_copy(cols[j], k) for j in range(k + 1, 8)]
            top = [row_copy(x, k) for x in own]
            for j in range(k + 1, 8):
                cols[j] = cols[j] - m * crossing[j - k - 1]
            own = [x - m * y for x, y in zip(own, top)]
            inverses.append(inverse)
            cross.append(crossing)
            tops.append(top)
        scale = lax.rsqrt(pivots)
        for t in range(1, tiles):
            work[tile(kb, t)] = own[t] * scale
        for g in range(kb + 1, order // 8):
            rest = [work[tile(g, t)] for t in range(tiles)]
            q = [lane_copy(rest[0], 8 * kb + j) for j in range(8)]
            for k in range(8):
                m = q[k] * inverses[k]
                for j in range(k + 1, 8):
                    q[j] = q[j] - m * cross[k][j - k - 1]
                rest = [x - m * y for x, y in zip(rest, tops[k])]
            for t in range(tiles):
                work[tile(g, t)] = rest[t]


def solve(metric, image, work):
    order, width = image.shape
    work[:, :order] = metric
    work[:, order : order + width] = image
    eliminate(work, (order + width) // 128)
    return work[:, order : order + width]


def finish_kernel(gram_ref, high_ref, low_ref, out_ref, work, out, sems):
    keep = out_ref.shape[0]
    g11, g12, g22 = unpack(gram_ref)
    square = exact(g11, g11)
    span = solve(exact(square, g11, NT), square, work)
    one = solve(exact(exact(span, g11), span, NT), span, work)
    cross = exact(exact(one, g12), one, NT)
    tail = exact(exact(one, g22), one, NT)
    same = jnp.where(places(keep) == 0, 1.0, 0.0)
    top = jnp.concatenate([same, cross], axis=1)
    bottom = jnp.concatenate([cross.T, tail], axis=1)
    gram = jnp.concatenate([top, bottom], axis=0)
    span = exact(top, gram)
    image = jnp.concatenate([exact(span[:, :keep], one), exact(span[:, keep:], one)], axis=1)
    overall = solve(exact(exact(span, gram), span, NT), image, work)
    fh, fl = split(overall)
    both = jnp.concatenate([fh, fl], axis=0)

    quarter = out.shape[1] // 4
    stores = []
    for b in range(out.shape[1] // WB):
        place = slice(b * WB, b * WB + WB)
        wide = mm(both, high_ref[:, place])
        out[:, place] = wide[:keep] + wide[keep:] + mm(fh, low_ref[:, place])
        if (b + 1) * WB % quarter == 0:
            at = pl.ds((b + 1) * WB - quarter, quarter)
            sem = sems.at[len(stores)]
            stores.append(pltpu.make_async_copy(out.at[:, at], out_ref.at[:, at], sem))
            stores[-1].start()
    for store in stores:
        store.wait()


def sum_kernel(in_ref, out_ref):
    total = in_ref[0]
    for i in range(1, in_ref.shape[0]):
        total = total + in_ref[i]
    for i in range(out_ref.shape[0]):
        out_ref[i] = total


def exchange(blocks, axis):
    return lax.all_to_all(blocks, axis, 0, 0, tiled=True)


def summed_copies(blocks, axis):
    copies = pl.pallas_call(
        sum_kernel,
        out_shape=jax.ShapeDtypeStruct((lax.axis_size(axis), *blocks.shape[1:]), jnp.float32),
        compiler_params=pltpu.CompilerParams(vmem_limit_bytes=8 * 1024 * 1024),
        name="sums_" + axis,
    )(blocks)
    return exchange(copies, axis)


def body(source, band_values, offsets):
    devices = lax.axis_size(ROWS)
    group = lax.axis_size("far")
    rows, width = source.shape
    reach = 3 * HB
    inner = width // WB
    up = [(i, i + 1) for i in range(devices - 1)]
    down = [(i + 1, i) for i in range(devices - 1)]

    hbm = pl.BlockSpec(memory_space=pltpu.HBM)
    vmem = pl.BlockSpec(memory_space=pltpu.VMEM)
    edge = jax.ShapeDtypeStruct((rows, reach + 2 * WB), jnp.float32)
    last, first = pl.pallas_call(
        edges_kernel,
        out_shape=[edge, edge],
        in_specs=[hbm, hbm],
        scratch_shapes=[pltpu.SemaphoreType.DMA((6,))],
        compiler_params=pltpu.CompilerParams(vmem_limit_bytes=4 * 1024 * 1024),
        name="edges",
    )(*[pltpu.with_memory_space_constraint(x, pltpu.HBM) for x in (source, band_values)])
    low = lax.ppermute(last, ROWS, up)
    high = lax.ppermute(first, ROWS, down)
    offsets = offsets.reshape(1, -1)
    blocks = jax.ShapeDtypeStruct((inner, SPAN, WB), jnp.bfloat16)
    stacked = jax.ShapeDtypeStruct((2 * rows, width), jnp.bfloat16)
    by_high, by_low, inside, once = pl.pallas_call(
        blocks_kernel,
        out_shape=[blocks, blocks, stacked, stacked],
        scratch_shapes=[
            pltpu.VMEM((2, WB, 2 * HB), jnp.bfloat16),
            pltpu.VMEM((2, WB, 2 * HB), jnp.float32),
            pltpu.VMEM((2, WB, 2 * HB), jnp.float32),
        ],
        compiler_params=pltpu.CompilerParams(vmem_limit_bytes=12 * 1024 * 1024),
        cost_estimate=pl.CostEstimate(
            flops=10_000_000_000, bytes_accessed=12_000_000, transcendentals=0
        ),
        name="blocks",
    )(band_values, offsets, source)
    wide = width + 2 * reach
    high, low, gram = pl.pallas_call(
        functools.partial(powers_kernel, float(width * devices)),
        out_shape=[
            jax.ShapeDtypeStruct((4 * rows, width), jnp.bfloat16),
            jax.ShapeDtypeStruct((4 * rows, width), jnp.bfloat16),
            jax.ShapeDtypeStruct((4 * rows + 16, 2 * rows), jnp.float32),
        ],
        scratch_shapes=[
            pltpu.VMEM((3, 2 * rows, wide), jnp.bfloat16),
            pltpu.VMEM((2, SPAN, WB), jnp.bfloat16),
            pltpu.VMEM((2, SPAN, WB), jnp.bfloat16),
            pltpu.VMEM((2, WB, 2 * HB), jnp.float32),
        ],
        compiler_params=pltpu.CompilerParams(vmem_limit_bytes=16 * 1024 * 1024),
        name="powers",
    )(inside, once, low, high, offsets, by_high, by_low)

    gram = exchange(gram.reshape(group, -1, 1, 2 * rows), "far")
    gram = summed_copies(summed_copies(gram, "near"), "far")
    gram = gram.reshape(4 * rows + 16, 2 * rows)

    return pl.pallas_call(
        finish_kernel,
        out_shape=jax.ShapeDtypeStruct((2 * rows, width), jnp.float32),
        out_specs=hbm,
        scratch_shapes=[
            pltpu.VMEM((2 * rows, 6 * rows), jnp.float32),
            pltpu.VMEM((2 * rows, width), jnp.float32),
            pltpu.SemaphoreType.DMA((4,)),
        ],
        compiler_params=pltpu.CompilerParams(vmem_limit_bytes=16 * 1024 * 1024),
        name="finish",
    )(gram, high, low)


def solution(mesh):
    devices = mesh.devices.size
    near = 1 << (devices.bit_length() // 2)
    grid = Mesh(mesh.devices.reshape(devices // near, near), ROWS)
    split_rows = P(None, ROWS)
    return jax.shard_map(
        body,
        mesh=grid,
        in_specs=(split_rows, split_rows, P()),
        out_specs=split_rows,
        check_vma=False,
    )
```

```python
import functools

import jax
import jax.numpy as jnp
from jax import lax
from jax.experimental import pallas as pl
from jax.experimental.pallas import tpu as pltpu
from jax.sharding import Mesh
from jax.sharding import PartitionSpec as P

HB = 128
WB = 256
SPAN = 2 * WB
ROWS = ("far", "near")
NN = (((1,), (0,)), ((), ()))
NT = (((1,), (1,)), ((), ()))


def split(x):
    high = x.astype(jnp.bfloat16)
    return high, (x - high.astype(jnp.float32)).astype(jnp.bfloat16)


def mm(a, b, dims=NN):
    return lax.dot_general(a, b, dims, preferred_element_type=jnp.float32)


def exact(a, b, dims=NN):
    return lax.dot_general(
        a, b, dims, precision=lax.Precision.HIGHEST, preferred_element_type=jnp.float32
    )


def picker(off_ref):
    count = off_ref.shape[1]
    down = lax.broadcasted_iota(jnp.int32, (2 * HB, count), 0)
    pick = jnp.where(down == off_ref[...] + HB, 1.0, 0.0).astype(jnp.bfloat16)
    last = jnp.where(off_ref[...] == HB, 1.0, 0.0)
    last = jnp.sum(jnp.where(places(count) == 0, last, 0.0), axis=1, keepdims=True)
    return jnp.concatenate([pick, pick], axis=1), last


def turned(values):
    return jnp.concatenate(split(values.T), axis=1)


def quarters():
    for half in range(2):
        for t in range(2):
            yield slice(half * HB, half * HB + HB), slice(t * HB, t * HB + HB)


def skew(diag, ref):
    for rows, lanes in quarters():
        ref[rows, lanes] = pltpu.roll(diag[rows, lanes], 0, 1, stride=1, stride_axis=0)


def place_block(rolled, last, wh, wl, b):
    beyond = places(HB)
    parts = [rolled[rows, lanes].T for rows, lanes in quarters()]
    for half in range(2):
        rows = slice(half * HB, half * HB + HB)
        near, far = parts[2 * half : 2 * half + 2]
        edge = jnp.where(beyond == 0, last[:, rows], 0.0)
        tiles = [
            jnp.where(beyond <= 0, near, 0.0),
            jnp.where(beyond <= 0, far, near),
            jnp.where(beyond > 0, far, edge),
        ]
        for t, tile in enumerate(tiles):
            high, low = split(tile)
            for ref, part in ((wh, high), (wl, low)):
                ref[b, (half + t) * HB : (half + t + 1) * HB, rows] = part
        empty = 3 * HB * (1 - half)
        for ref in (wh, wl):
            ref[b, empty : empty + HB, rows] = jnp.zeros((HB, HB), jnp.bfloat16)


def final(values, last):
    return jnp.sum(values * last, axis=0, keepdims=True)


def blocks_kernel(
    band_ref, off_ref, src_ref, wh, wl, s_ref, a_ref, both_ref, diag_ref, rolled_ref
):
    pick, last = picker(off_ref)
    count = wh.shape[0]
    rows = src_ref.shape[0]
    for b in range(count + 3):
        if 5 <= b:
            k = b - 4
            pair = applied(s_ref[:, k * WB - HB : k * WB - HB + SPAN], wh[k], wl[k])
            for part in range(2):
                a_ref[part * rows : (part + 1) * rows, k * WB : k * WB + WB] = pair[part]
        if 3 <= b:
            values = band_ref[:, (b - 3) * WB : (b - 2) * WB]
            place_block(rolled_ref[(b - 3) % 2], final(values, last), wh, wl, b - 3)
        if 2 <= b < count + 2:
            skew(diag_ref[(b - 2) % 2], rolled_ref.at[(b - 2) % 2])
        if 1 <= b < count + 1:
            diag_ref[(b - 1) % 2] = mm(both_ref[(b - 1) % 2], pick, NT)
        if b < count:
            at = slice(b * WB, b * WB + WB)
            both_ref[b % 2] = turned(band_ref[:, at])
            s_ref[:rows, at], s_ref[rows:, at] = split(src_ref[:, at])


def applied(window, by_high, by_low):
    rows = window.shape[0] // 2
    both = mm(window, by_high)
    return split(both[:rows] + both[rows:] + mm(window[:rows], by_low))


def edges_kernel(src_ref, band_ref, up_ref, down_ref, sems):
    rows, width = src_ref.shape
    reach = 3 * HB
    copies = []
    for ref, far, near in ((up_ref, width - reach, width - WB), (down_ref, 0, 0)):
        parts = [(src_ref.at[:, pl.ds(far, reach)], ref.at[:, pl.ds(0, reach)])]
        for half in range(2):
            take = band_ref.at[pl.ds(half * rows, rows), pl.ds(near, WB)]
            parts.append((take, ref.at[:, pl.ds(reach + half * WB, WB)]))
        for one, two in parts:
            copies.append(pltpu.make_async_copy(one, two, sems.at[len(copies)]))
    for copy in copies:
        copy.start()
    for copy in copies:
        copy.wait()


def powers_kernel(
    total, s_ref, a_ref, low_in, high_in, off_ref, wh, wl, high_ref, low_ref, gram_ref, xs, eh, el, rolled
):
    rows, width = s_ref.shape[0] // 2, s_ref.shape[1]
    inner = width // WB
    reach = 3 * HB
    edges = [(low_in, 0, 0), (high_in, 1, reach + width)]
    for b in range(inner):
        at = slice(b * WB, b * WB + WB)
        into = slice(b * WB + reach, b * WB + reach + WB)
        high_ref[:rows, at] = s_ref[:rows, at]
        low_ref[:rows, at] = s_ref[rows:, at]
        xs[0, :, into] = s_ref[:, at]
    pick, last = picker(off_ref)
    sides = []
    for ref, side, at in edges:
        high, low = split(ref[:, :reach])
        xs[0, :rows, at : at + reach] = high
        xs[0, rows:, at : at + reach] = low
        values = jnp.concatenate([ref[:, reach : reach + WB], ref[:, reach + WB :]], axis=0)
        sides.append((values, mm(turned(values), pick, NT)))
    for side, (values, diag) in enumerate(sides):
        skew(diag, rolled.at[side])
    for side, (values, diag) in enumerate(sides):
        place_block(rolled[side], final(values, last), eh, el, side)
    for power in (1, 2):
        for at in (0, xs.shape[2] - HB):
            xs[power, :, at : at + HB] = jnp.zeros((2 * rows, HB), jnp.bfloat16)

    for power in (1, 2, 3):
        inside = list(range(2, inner)) + [1, inner]
        for b in inside + [0, inner + 1] * (power < 3):
            if b in (0, inner + 1):
                by = (eh[int(b > 0)], el[int(b > 0)])
            else:
                by = (wh[b - 1], wl[b - 1])
            if power == 1 and 1 < b < inner:
                at = slice(b * WB - WB, b * WB)
                pair = a_ref[:rows, at], a_ref[rows:, at]
            else:
                pair = applied(xs[power - 1, :, b * WB : b * WB + SPAN], *by)
            if power < 3:
                for part in range(2):
                    place = slice(b * WB + HB, b * WB + HB + WB)
                    xs[power, part * rows : (part + 1) * rows, place] = pair[part]
            if 0 < b <= inner:
                for ref, value in zip((high_ref, low_ref), pair):
                    ref[power * rows : (power + 1) * rows, b * WB - WB : b * WB] = value
    tall = high_ref[...]
    gram = mm(tall, tall, NT) + 2.0 * mm(tall, low_ref[...], NT)
    pack(gram_ref, (gram + gram.T) * (0.5 / total))


def places(order):
    shape = (order, order)
    down = lax.broadcasted_iota(jnp.int32, shape, 0)
    return lax.broadcasted_iota(jnp.int32, shape, 1) - down


def pack(ref, gram):
    half = ref.shape[1]
    across = places(half)
    tail = gram[half:, half:]
    ref[:half] = gram[:half, half:]
    ref[half : 2 * half] = jnp.where(across >= 0, gram[:half, :half], tail)
    ref[2 * half :] = jnp.zeros((ref.shape[0] - 2 * half, half), jnp.float32)
    middle = jnp.sum(jnp.where(across == 0, tail, 0.0), axis=0, keepdims=True)
    ref[2 * half : 2 * half + 1] = middle


def unpack(ref):
    half = ref.shape[1]
    across = places(half)
    cross = ref[:half]
    both = ref[half : 2 * half]
    middle = jnp.broadcast_to(ref[2 * half : 2 * half + 1], (half, half))
    upper = jnp.where(across > 0, both, 0.0)
    lower = jnp.where(across < 0, both, 0.0)
    head = upper + upper.T + jnp.where(across == 0, both, 0.0)
    tail = lower + lower.T + jnp.where(across == 0, middle, 0.0)
    return head, cross, tail


def lane_copy(x, lane):
    return jnp.broadcast_to(x[:, lane : lane + 1], (8, 128))


def row_copy(x, row):
    return jnp.broadcast_to(x[row : row + 1, :], (8, 128))


def eliminate(work, tiles):
    order = work.shape[0]
    sub = lax.broadcasted_iota(jnp.int32, (8, 128), 0)

    def tile(g, t):
        return slice(8 * g, 8 * g + 8), slice(128 * t, 128 * t + 128)

    for kb in range(order // 8):
        own = [work[tile(kb, t)] for t in range(tiles)]
        cols = [lane_copy(own[0], 8 * kb + j) for j in range(8)]
        inverses, cross, tops = [], [], []
        pivots = jnp.ones((8, 128), jnp.float32)
        for k in range(8):
            pivot = row_copy(cols[k], k)
            inverse = 1.0 / pivot
            pivots = jnp.where(sub == k, pivot, pivots)
            m = jnp.where(sub > k, cols[k] * inverse, 0.0)
            crossing = [row_copy(cols[j], k) for j in range(k + 1, 8)]
            top = [row_copy(x, k) for x in own]
            for j in range(k + 1, 8):
                cols[j] = cols[j] - m * crossing[j - k - 1]
            own = [x - m * y for x, y in zip(own, top)]
            inverses.append(inverse)
            cross.append(crossing)
            tops.append(top)
        scale = lax.rsqrt(pivots)
        for t in range(tiles):
            work[tile(kb, t)] = own[t] * scale
        for g in range(kb + 1, min(8 * (kb // 8) + 8 + 0, order // 8)):
            rest = [work[tile(g, t)] for t in range(tiles)]
            q = [lane_copy(rest[0], 8 * kb + j) for j in range(8)]
            for k in range(8):
                m = q[k] * inverses[k]
                for j in range(k + 1, 8):
                    q[j] = q[j] - m * cross[k][j - k - 1]
                rest = [x - m * y for x, y in zip(rest, tops[k])]
            for t in range(tiles):
                work[tile(g, t)] = rest[t]
        done = 8 * kb + 8
        start = done + 8 * 0
        if done % 64 == 0 and start < order:
            panel = work[done - 64 : done, :]
            rest = exact(panel[:, start:order], panel, (((0,), (0,)), ((), ())))
            work[start:order, :] = work[start:order, :] - rest


def solve(metric, image, work):
    order, width = image.shape
    work[:, :order] = metric
    work[:, order : order + width] = image
    eliminate(work, (order + width) // 128)
    return work[:, order : order + width]


def finish_kernel(gram_ref, high_ref, low_ref, out_ref, work, out, sems):
    keep = out_ref.shape[0]
    g11, g12, g22 = unpack(gram_ref)
    square = exact(g11, g11)
    span = solve(exact(square, g11, NT), square, work)
    one = solve(exact(exact(span, g11), span, NT), span, work)
    cross = exact(exact(one, g12), one, NT)
    tail = exact(exact(one, g22), one, NT)
    same = jnp.where(places(keep) == 0, 1.0, 0.0)
    top = jnp.concatenate([same, cross], axis=1)
    bottom = jnp.concatenate([cross.T, tail], axis=1)
    gram = jnp.concatenate([top, bottom], axis=0)
    span = exact(top, gram)
    image = jnp.concatenate([exact(span[:, :keep], one), exact(span[:, keep:], one)], axis=1)
    overall = solve(exact(exact(span, gram), span, NT), image, work)
    fh, fl = split(overall)
    both = jnp.concatenate([fh, fl], axis=0)

    quarter = out.shape[1] // 4
    stores = []
    for b in range(out.shape[1] // WB):
        place = slice(b * WB, b * WB + WB)
        wide = mm(both, high_ref[:, place])
        out[:, place] = wide[:keep] + wide[keep:] + mm(fh, low_ref[:, place])
        if (b + 1) * WB % quarter == 0:
            at = pl.ds((b + 1) * WB - quarter, quarter)
            sem = sems.at[len(stores)]
            stores.append(pltpu.make_async_copy(out.at[:, at], out_ref.at[:, at], sem))
            stores[-1].start()
    for store in stores:
        store.wait()


def sum_kernel(in_ref, out_ref):
    total = in_ref[0]
    for i in range(1, in_ref.shape[0]):
        total = total + in_ref[i]
    for i in range(out_ref.shape[0]):
        out_ref[i] = total


def exchange(blocks, axis):
    return lax.all_to_all(blocks, axis, 0, 0, tiled=True)


def summed_copies(blocks, axis):
    copies = pl.pallas_call(
        sum_kernel,
        out_shape=jax.ShapeDtypeStruct((lax.axis_size(axis), *blocks.shape[1:]), jnp.float32),
        compiler_params=pltpu.CompilerParams(vmem_limit_bytes=8 * 1024 * 1024),
        name="sums_" + axis,
    )(blocks)
    return exchange(copies, axis)


def body(source, band_values, offsets):
    devices = lax.axis_size(ROWS)
    group = lax.axis_size("far")
    rows, width = source.shape
    reach = 3 * HB
    inner = width // WB
    up = [(i, i + 1) for i in range(devices - 1)]
    down = [(i + 1, i) for i in range(devices - 1)]

    hbm = pl.BlockSpec(memory_space=pltpu.HBM)
    vmem = pl.BlockSpec(memory_space=pltpu.VMEM)
    edge = jax.ShapeDtypeStruct((rows, reach + 2 * WB), jnp.float32)
    last, first = pl.pallas_call(
        edges_kernel,
        out_shape=[edge, edge],
        in_specs=[hbm, hbm],
        scratch_shapes=[pltpu.SemaphoreType.DMA((6,))],
        compiler_params=pltpu.CompilerParams(vmem_limit_bytes=4 * 1024 * 1024),
        name="edges",
    )(*[pltpu.with_memory_space_constraint(x, pltpu.HBM) for x in (source, band_values)])
    low = lax.ppermute(last, ROWS, up)
    high = lax.ppermute(first, ROWS, down)
    offsets = offsets.reshape(1, -1)
    blocks = jax.ShapeDtypeStruct((inner, SPAN, WB), jnp.bfloat16)
    stacked = jax.ShapeDtypeStruct((2 * rows, width), jnp.bfloat16)
    by_high, by_low, inside, once = pl.pallas_call(
        blocks_kernel,
        out_shape=[blocks, blocks, stacked, stacked],
        scratch_shapes=[
            pltpu.VMEM((2, WB, 2 * HB), jnp.bfloat16),
            pltpu.VMEM((2, WB, 2 * HB), jnp.float32),
            pltpu.VMEM((2, WB, 2 * HB), jnp.float32),
        ],
        compiler_params=pltpu.CompilerParams(vmem_limit_bytes=12 * 1024 * 1024),
        cost_estimate=pl.CostEstimate(
            flops=10_000_000_000, bytes_accessed=12_000_000, transcendentals=0
        ),
        name="blocks",
    )(band_values, offsets, source)
    wide = width + 2 * reach
    high, low, gram = pl.pallas_call(
        functools.partial(powers_kernel, float(width * devices)),
        out_shape=[
            jax.ShapeDtypeStruct((4 * rows, width), jnp.bfloat16),
            jax.ShapeDtypeStruct((4 * rows, width), jnp.bfloat16),
            jax.ShapeDtypeStruct((4 * rows + 16, 2 * rows), jnp.float32),
        ],
        scratch_shapes=[
            pltpu.VMEM((3, 2 * rows, wide), jnp.bfloat16),
            pltpu.VMEM((2, SPAN, WB), jnp.bfloat16),
            pltpu.VMEM((2, SPAN, WB), jnp.bfloat16),
            pltpu.VMEM((2, WB, 2 * HB), jnp.float32),
        ],
        compiler_params=pltpu.CompilerParams(vmem_limit_bytes=16 * 1024 * 1024),
        name="powers",
    )(inside, once, low, high, offsets, by_high, by_low)

    gram = exchange(gram.reshape(group, -1, 1, 2 * rows), "far")
    gram = summed_copies(summed_copies(gram, "near"), "far")
    gram = gram.reshape(4 * rows + 16, 2 * rows)

    return pl.pallas_call(
        finish_kernel,
        out_shape=jax.ShapeDtypeStruct((2 * rows, width), jnp.float32),
        out_specs=hbm,
        scratch_shapes=[
            pltpu.VMEM((2 * rows, 6 * rows), jnp.float32),
            pltpu.VMEM((2 * rows, width), jnp.float32),
            pltpu.SemaphoreType.DMA((4,)),
        ],
        compiler_params=pltpu.CompilerParams(vmem_limit_bytes=16 * 1024 * 1024),
        name="finish",
    )(gram, high, low)


def solution(mesh):
    devices = mesh.devices.size
    near = 1 << (devices.bit_length() // 2)
    grid = Mesh(mesh.devices.reshape(devices // near, near), ROWS)
    split_rows = P(None, ROWS)
    return jax.shard_map(
        body,
        mesh=grid,
        in_specs=(split_rows, split_rows, P()),
        out_specs=split_rows,
        check_vma=False,
    )
```
